32 devices in a mesh: member: 2 (over y), tile: 8 (over z, x), sub: 2 (over core).
Axes of the slice: x: 2, y: 2, z: 4, core: 2. Of those that a mesh axis runs over, the one named last changes fastest.
Arguments:
- atm_state: bfloat16 [8, 32768], P(None, ('member', 'tile')), parts along dimension 1, may hold values from -6 to 6
- ocn_state: bfloat16 [4, 32768], P(None, ('member', 'tile', 'sub')), parts along dimension 1, may hold values from -6 to 6
- need_atm: int32 [128], P(('tile', 'sub')), may hold values from 0 to 127, as said below
- xb_need: int32 [128], P(('tile', 'sub')), may hold values from 0 to 15
- xb_ocn: int32 [128], P(('tile', 'sub')), may hold values from 0 to 15
- xb_count: int32 [16], P(('tile', 'sub')), may hold values from 1 to 8, as said below
- sea_mask: int32 [16384], P(('tile', 'sub')), may hold values 0 or 1
- cell_area: float32 [16384], P(('tile', 'sub')), may hold values from 0.5 to 2
- w_atm: bfloat16 [128, 128, 128], P(('tile', 'sub')), may hold values from 0.0099487305 to 1
- w_ocn: bfloat16 [128, 128, 128], P(('tile', 'sub')), may hold values from 0.0099487305 to 1
Outputs:
- atm_flux: float32 [4, 32768], P(None, ('member', 'tile')), parts along dimension 1
- ocn_flux: float32 [4, 32768], P(None, ('member', 'tile', 'sub')), parts along dimension 1
The draws below stay inside these ranges and needn't reach their ends.
There are 2 independent parts, one for each index of `member`. The reference program is written for one: setup_inputs(seed, part) draws one part's arguments, and reference() takes and returns one part's arrays. A program takes and returns all parts, laid end to end along the dimension named above; an argument that names none is the same for every part. Nothing has to cross between parts.
Inputs may be any that keep to these rules, and one draw needn't show every extreme that they name: `need_atm`: an atmosphere block n lies on tile n // 16. A tile's list is the entries of its devices in device order; for tile t its entries 2 i and 2 i + 1 lie on tile (t + i - 8 // 2 + 1) mod 8 for i < 7, and on tile (t + 4) mod 8 for i = 7; all entries of one tile's list are distinct. `xb_need`: index into the list of the block's tile. `xb_ocn`: index among the ocean blocks of the block's tile, in device order. `xb_count`: some device has all 8 blocks live.
All inputs are finite; a program needn't handle non-finite values. No bound on the sum of `sea_mask` on one device may be relied on, other than what follows from the above.
Results may differ from the reference program's by a relative error of at most 0.0003.
Values may be sent and summed in bfloat16 or wider, within the bound.
A program may use at most 64 MiB of HBM per device.

```python
import math
import jax
import jax.numpy as jnp
from jax import lax

F_A = 8
F_O = 4
F_X = 4
BLK = 128
ABLK_TILE = 16
OBLK_DEV = 8
XB_DEV = 8
NEED_DEV = 8
ATM_CELLS = 16384
OCN_CELLS = 16384
XBLKS = 128
N_TILE = 8
N_SUB = 2


def draw_need_atm(key, part):
    first, second = jax.random.split(key, 2)
    lower = jax.random.randint(first, (N_TILE, NEED_DEV), 0, ABLK_TILE)
    apart = jax.random.randint(second, (N_TILE, NEED_DEV), 1, ABLK_TILE)
    upper = (lower + apart) % ABLK_TILE
    locals_pair = jnp.stack([lower, upper], 2)
    order = jnp.arange(NEED_DEV, dtype=jnp.int32)
    offset = jnp.where(order < NEED_DEV - 1, order - NEED_DEV // 2 + 1, N_TILE // 2)
    owner = (jnp.arange(N_TILE, dtype=jnp.int32)[:, None] + offset[None, :]) % N_TILE
    return (owner[:, :, None] * ABLK_TILE + locals_pair).reshape(-1).astype(jnp.int32)


def draw_xb_count(key, part):
    devices = N_TILE * N_SUB
    shifts = jax.random.randint(key, (devices,), 0, 3)
    chosen = jax.random.randint(jax.random.fold_in(key, 7), (), 0, devices)
    shifts = jnp.where(jnp.arange(devices) == chosen, 0, shifts)
    return (XB_DEV // jnp.left_shift(1, shifts)).astype(jnp.int32)


def with_ends(array, own_key, least, largest):
    dims = array.shape
    place = [jax.random.randint(jax.random.fold_in(own_key, axis), (), 0, dims[axis]) for axis in range(len(dims))]
    array = array.at[tuple(place)].set(least)
    longest = dims.index(max(dims))
    place[longest] = (place[longest] + 1) % dims[longest]
    return array.at[tuple(place)].set(largest)


def block_scale(key, extent, cuts, smallest, top_value):
    level = 1.0
    for position, shards_of in cuts:
        steps = jax.random.uniform(jax.random.fold_in(jax.random.fold_in(key, 6), position), (shards_of,), jnp.float32, smallest / len(cuts), top_value / len(cuts))
        level = level * jnp.repeat(jnp.exp(steps), extent[position] // shards_of).reshape((-1,) + (1,) * (len(extent) - 1 - position))
    return level


def scatter_about(rng, dims, spread, limit, cuts=(), kind=jnp.bfloat16):
    level = block_scale(rng, dims, cuts, -0.22, 0.18) if cuts else 1.0
    entries = jax.random.normal(rng, dims, jnp.float32) * spread * level
    return jnp.minimum(jnp.maximum(entries, -limit), limit).astype(kind)


def setup_inputs(seed: int = 0, part: int = 0) -> dict:
    key_list = jax.random.split(jax.random.key(seed), 11)
    own_keys = jax.random.split(jax.random.fold_in(key_list[10], part), 11)
    return {
        "atm_state": scatter_about(own_keys[0], (F_A, ATM_CELLS), 1.0, 6.0, ((1, 8),)),
        "ocn_state": scatter_about(own_keys[1], (F_O, OCN_CELLS), 1.0, 6.0, ((1, 16),)),
        "need_atm": draw_need_atm(jax.random.fold_in(key_list[10], 71), part),
        "xb_need": with_ends(jax.random.randint(key_list[3], (XBLKS,), 0, N_SUB * NEED_DEV), jax.random.fold_in(key_list[3], 1), 0, (N_SUB * NEED_DEV) - 1).astype(jnp.int32),
        "xb_ocn": with_ends(jax.random.randint(key_list[4], (XBLKS,), 0, N_SUB * OBLK_DEV), jax.random.fold_in(key_list[4], 1), 0, (N_SUB * OBLK_DEV) - 1).astype(jnp.int32),
        "xb_count": draw_xb_count(jax.random.fold_in(key_list[10], 71), part),
        "sea_mask": with_ends((jax.random.randint(key_list[6], (XBLKS * BLK,), 0, 3) < 2).astype(jnp.int32), jax.random.fold_in(key_list[6], 1), 0, 1),
        "cell_area": jnp.clip(jnp.exp(math.log(2.0) - 1.3862944 * jax.random.uniform(key_list[7], (XBLKS * BLK,), jnp.float32) ** block_scale(key_list[7], (XBLKS * BLK,), ((0, 16),), -0.2, 0.2)), 0.5, 2.0),
        "w_atm": jnp.clip(jnp.exp(math.log(1.0) - 4.61031033 * jax.random.uniform(key_list[8], (XBLKS, BLK, BLK), jnp.float32) ** block_scale(key_list[8], (XBLKS, BLK, BLK), ((0, 16),), -0.2, 0.2)), 0.0099487305, 1.0).astype(jnp.bfloat16),
        "w_ocn": jnp.clip(jnp.exp(math.log(1.0) - 4.61031033 * jax.random.uniform(key_list[9], (XBLKS, BLK, BLK), jnp.float32) ** block_scale(key_list[9], (XBLKS, BLK, BLK), ((0, 16),), -0.2, 0.2)), 0.0099487305, 1.0).astype(jnp.bfloat16),
    }


def bulk_fluxes(upper_domain_vector, marine_regrid_transfer):
    lowest_level_warmth, vapour_mixing_ratio, eastward_wind, northward_wind, ground_level_pressure, solar_radiation, infrared_radiation, rainfall_rate = [upper_domain_vector[:, grid_box_number] for grid_box_number in range(8)]
    skin_warmth_kelvin, eastward_current, northward_current, marine_climate_coupler = [marine_regrid_transfer[:, grid_box_number] for grid_box_number in range(4)]
    du = eastward_wind - eastward_current
    dv = northward_wind - northward_current
    speed = jnp.sqrt(du * du + dv * dv + 1.0)
    momentum_transfer_factor = (0.3 + 0.1 * jnp.tanh(ground_level_pressure)) * speed
    conductive_energy_loss = momentum_transfer_factor * (skin_warmth_kelvin - lowest_level_warmth)
    evaporative_energy_loss = momentum_transfer_factor * (0.5 * skin_warmth_kelvin - vapour_mixing_ratio)
    taux = momentum_transfer_factor * du
    tauy = momentum_transfer_factor * dv
    reflected_fraction = 0.06 + 0.1 * jax.nn.sigmoid(marine_climate_coupler)
    thermal_energy_transfer = (1.0 - reflected_fraction) * solar_radiation + infrared_radiation - 0.2 * skin_warmth_kelvin - conductive_energy_loss - evaporative_energy_loss
    fresh = rainfall_rate - 0.5 * evaporative_energy_loss
    return (jnp.stack([conductive_energy_loss, evaporative_energy_loss, taux, tauy], 1), jnp.stack([thermal_energy_transfer, taux, tauy, fresh], 1))

def reference(atm_state, ocn_state, need_atm, xb_need, xb_ocn, xb_count, sea_mask, cell_area, w_atm, w_ocn):
    devices = N_TILE * N_SUB
    highest = lax.Precision.HIGHEST
    atm_table = jnp.transpose(atm_state.reshape(F_A, N_TILE * ABLK_TILE, BLK), (1, 0, 2))
    ocn_table = jnp.transpose(ocn_state.reshape(F_O, devices * OBLK_DEV, BLK), (1, 0, 2))
    list_len = N_SUB * NEED_DEV
    items = (jnp.arange(devices, dtype=jnp.int32), xb_need.reshape(devices, XB_DEV), xb_ocn.reshape(devices, XB_DEV), xb_count, sea_mask.reshape(devices, XB_DEV, BLK), cell_area.reshape(devices, XB_DEV, BLK), w_atm.reshape(devices, XB_DEV, BLK, BLK), w_ocn.reshape(devices, XB_DEV, BLK, BLK))

    def step(carry, item):
        acc_atm, acc_ocn = carry
        device, need_idx, ocn_idx, count, sea, area, weight_a, weight_o = item
        tile = device // N_SUB
        tile_list = lax.dynamic_slice_in_dim(need_atm, (tile * list_len).astype(jnp.int32), list_len)
        ids = tile_list[need_idx]
        oids = (tile * (N_SUB * OBLK_DEV) + ocn_idx).astype(jnp.int32)
        wa = weight_a.astype(jnp.float32)
        wo = weight_o.astype(jnp.float32)
        upper_domain_vector = jnp.einsum('bfj,bxj->bfx', atm_table[ids].astype(jnp.float32), wa, precision=highest) / lax.optimization_barrier(jnp.sum(wa, 2))[:, None, :]
        marine_regrid_transfer = jnp.einsum('bfj,bxj->bfx', ocn_table[oids].astype(jnp.float32), wo, precision=highest) / lax.optimization_barrier(jnp.sum(wo, 2))[:, None, :]
        to_atm, to_ocn = bulk_fluxes(upper_domain_vector, marine_regrid_transfer)
        live = (jnp.arange(XB_DEV, dtype=jnp.int32) < count).astype(jnp.float32)[:, None]
        weighted = area * live
        wet = weighted * sea.astype(jnp.float32)
        atm_terms = jnp.concatenate([to_atm * wet[:, None, :], weighted[:, None, :]], 1)
        ocn_terms = jnp.concatenate([to_ocn * wet[:, None, :], wet[:, None, :]], 1)
        atm_cells = jnp.einsum('bgx,bxj->bgj', atm_terms, wa, precision=highest)
        ocn_cells = jnp.einsum('bgx,bxj->bgj', ocn_terms, wo, precision=highest)
        return ((acc_atm.at[ids].add(atm_cells), acc_ocn.at[oids].add(ocn_cells)), None)
    init = (jnp.zeros((N_TILE * ABLK_TILE, F_X + 1, BLK), jnp.float32), jnp.zeros((devices * OBLK_DEV, F_X + 1, BLK), jnp.float32))
    (acc_atm, acc_ocn), _ = lax.scan(step, init, items)
    atm_flux = acc_atm[:, :F_X] / jnp.maximum(acc_atm[:, F_X:], 1.0)
    ocn_flux = acc_ocn[:, :F_X] / jnp.maximum(acc_ocn[:, F_X:], 1.0)
    atm_flux = jnp.transpose(atm_flux, (1, 0, 2)).reshape(F_X, N_TILE * ABLK_TILE * BLK)
    ocn_flux = jnp.transpose(ocn_flux, (1, 0, 2)).reshape(F_X, devices * OBLK_DEV * BLK)
    return (atm_flux, ocn_flux)
```

```python
import functools

import jax
import jax.numpy as jnp
from jax import lax
from jax.experimental import pallas as pl
from jax.experimental.pallas import tpu as pltpu
from jax.sharding import PartitionSpec as P

MESH = pl.DeviceIdType.MESH
ROWS = 8
PAIR = 2
F32 = jnp.float32
BF16 = jnp.bfloat16
TRANSPOSED = (((1,), (1,)), ((), ()))


def split(value):
    high = value.astype(BF16)
    low = (value - high.astype(F32)).astype(BF16)
    return high, low


def kernel(
    ntile, nsub, blk,
    state_hbm, ocean_hbm, need_hbm, xbn_hbm, xbo_hbm, count_hbm, sea_hbm, area_hbm, wa_hbm, wo_hbm,
    atm_out, ocn_out,
    state, octab, need, xbn, xbo, count, sea, area, wa, wo,
    table, picked, rows_send, rows_recv, sums_send, sums_recv, oc_send, oc_recv, atm_v, ocn_v,
    load_sem, block_sem, push_ssem, push_rsem, row_ssem, row_rsem, oc_ssem, oc_rsem,
    pick_ssem, pick_rsem, sum_ssem, sum_rsem, ob_ssem, ob_rsem, out_sem,
):
    me = lax.axis_index("tile")
    core = lax.axis_index("sub")
    other = 1 - core
    nb = wa.shape[0]
    mine = need.shape[0]
    half = mine // PAIR
    owners = half * nsub
    entries = mine * nsub
    owned = state.shape[0]
    obl = octab.shape[1]
    nflux = atm_v.shape[0]

    def offset(i):
        return ntile // 2 if i == owners - 1 else i - owners // 2 + 1

    def tile_at(delta):
        return lax.rem(me + delta + ntile, ntile)

    zero_i = [i for i in range(owners) if offset(i) == 0][0]

    local = [
        pltpu.make_async_copy(src, dst, load_sem.at[k])
        for k, (src, dst) in enumerate(
            [
                (need_hbm, need),
                (wo_hbm, wo),
                (wa_hbm, wa),
                (xbo_hbm, xbo),
                (xbn_hbm, xbn),
                (count_hbm, count),
                (sea_hbm, sea),
                (area_hbm, area),
            ]
        )
    ]
    blocks = [
        pltpu.make_async_copy(
            state_hbm.at[:, pl.ds(n * blk, blk)], state.at[n], block_sem.at[n]
        )
        for n in range(owned)
    ] + [
        pltpu.make_async_copy(
            ocean_hbm.at[:, pl.ds(n * blk, blk)], octab.at[core, n], block_sem.at[owned + n]
        )
        for n in range(obl)
    ]
    for copy in blocks + local:
        copy.start()

    barrier = pltpu.get_barrier_semaphore()
    for i in range(owners):
        for c in range(nsub):
            if i == zero_i:
                continue
            pl.semaphore_signal(
                barrier, inc=1, device_id={"tile": tile_at(offset(i)), "sub": c}, device_id_type=MESH
            )
    pl.semaphore_signal(barrier, inc=1, device_id={"tile": me, "sub": other}, device_id_type=MESH)

    local[0].wait()
    lane = lax.broadcasted_iota(jnp.int32, (1, blk), 1)
    odd = lax.rem(lane // ROWS, PAIR)
    for k in range(half):
        first = lax.rem(need[PAIR * k], owned)
        second = lax.rem(need[PAIR * k + 1], owned)
        rows_send[k] = jnp.where(odd == 0, first, second)
    for copy in blocks:
        copy.wait()
    pl.semaphore_wait(barrier, owners * nsub - 1)

    def delta_of(k):
        out = jnp.int32(0)
        for c in range(nsub):
            out = jnp.where(core == c, jnp.int32(offset(c * half + k)), out)
        return out

    deltas = [delta_of(k) for k in range(half)]
    pushes = [
        pltpu.make_async_remote_copy(
            src_ref=state,
            dst_ref=table.at[k],
            send_sem=push_ssem.at[k],
            recv_sem=push_rsem.at[k],
            device_id={"tile": tile_at(-deltas[k]), "sub": core},
            device_id_type=MESH,
        )
        for k in range(half)
    ]
    keep = pltpu.make_async_copy(state, table.at[zero_i % half], out_sem.at[0])
    zero_core = zero_i // half
    order = sorted(range(half), key=lambda k: -abs(offset(k)))
    for k in order:
        if k == zero_i % half:
            @pl.when(core == zero_core)
            def _():
                keep.start()

            @pl.when(core != zero_core)
            def _(k=k):
                pushes[k].start()
        else:
            pushes[k].start()
    oc_copy = pltpu.make_async_remote_copy(
        src_ref=octab.at[core],
        dst_ref=octab.at[core],
        send_sem=oc_ssem,
        recv_sem=oc_rsem,
        device_id={"tile": me, "sub": other},
        device_id_type=MESH,
    )
    oc_copy.start()

    row_copies = []
    for k in range(half):
        slot = core * half + k
        for c in range(nsub):
            row_copies.append(
                pltpu.make_async_remote_copy(
                    src_ref=rows_send.at[k],
                    dst_ref=rows_recv.at[slot],
                    send_sem=row_ssem.at[k * nsub + c],
                    recv_sem=row_rsem.at[slot],
                    device_id={"tile": tile_at(deltas[k]), "sub": c},
                    device_id_type=MESH,
                )
            )
            copy = row_copies[-1]
            if k == zero_i % half:
                here = jnp.logical_and(core == zero_core, core == c)

                @pl.when(here)
                def _(k=k):
                    rows_recv[zero_i] = rows_send[k]

                @pl.when(jnp.logical_not(here))
                def _(copy=copy):
                    copy.start()
            else:
                copy.start()

    ones = jnp.ones((ROWS, blk), BF16)
    local[1].wait()
    local[3].wait()
    oc_copy.wait_recv()
    oxs = []
    for b in range(nb):
        m = xbo[b]
        cells = octab[lax.div(m, obl), lax.rem(m, obl)]
        w = wo[b]
        top = lax.dot_general(cells, w, TRANSPOSED, preferred_element_type=F32)
        den = lax.dot_general(ones, w, TRANSPOSED, preferred_element_type=F32)
        oxs.append(top / den[: top.shape[0]])
    ox = jnp.concatenate(oxs, axis=1)
    sst, uo, vo, oa = [ox[f : f + 1] for f in range(4)]
    albedo = 0.06 + 0.05 * (1.0 + jnp.tanh(0.5 * oa))
    local[2].wait()
    dens = jnp.concatenate(
        [lax.dot_general(ones, wa[b], TRANSPOSED, preferred_element_type=F32) for b in range(nb)],
        axis=1,
    )
    rden = 1.0 / dens
    for k in (4, 5, 6, 7):
        local[k].wait()
    cell = lax.broadcasted_iota(jnp.int32, (1, nb * blk), 1)
    weighted = jnp.where(cell < count[0] * blk, area[...], 0.0)
    wet = weighted * sea[...].astype(F32)

    for k in range(half):
        if k == zero_i % half:
            @pl.when(core == zero_core)
            def _():
                keep.wait()

            @pl.when(core != zero_core)
            def _(k=k):
                pushes[k].wait_recv()
        else:
            pushes[k].wait_recv()
    for e in range(mine):
        picked[core * mine + e] = table[e // PAIR, lax.rem(need[e], owned)]
    part = picked.at[pl.ds(core * mine, mine)]
    pick_copy = pltpu.make_async_remote_copy(
        src_ref=part,
        dst_ref=part,
        send_sem=pick_ssem,
        recv_sem=pick_rsem,
        device_id={"tile": me, "sub": other},
        device_id_type=MESH,
    )
    pick_copy.start()
    pick_copy.wait_recv()
    ax = jnp.concatenate(
        [
            lax.dot_general(picked[xbn[b]], wa[b], TRANSPOSED, preferred_element_type=F32)
            for b in range(nb)
        ],
        axis=1,
    )
    ax = ax * rden
    ta, qa, ua, va, ps, sw, lw, pr = [ax[f : f + 1] for f in range(8)]

    du = ua - uo
    dv = va - vo
    speed = jnp.sqrt(du * du + dv * dv + 1.0)
    cd = (0.3 + 0.1 * jnp.tanh(ps)) * speed
    sens = cd * (sst - ta)
    lat = cd * (0.5 * sst - qa)
    taux = cd * du
    tauy = cd * dv
    pad = jnp.zeros((ROWS - 5, nb * blk), F32)
    atm_terms = jnp.concatenate([sens * wet, lat * wet, taux * wet, tauy * wet, weighted, pad], 0)
    both = jnp.concatenate(split(atm_terms), axis=0)

    def spread(both, w, index, number):
        totals = [None] * number
        for b in range(nb):
            prod = jnp.dot(both[:, b * blk : (b + 1) * blk], w[b], preferred_element_type=F32)
            prod = prod[:ROWS] + prod[ROWS:]
            at = jnp.full((ROWS, blk), index[b], jnp.int32)
            for n in range(number):
                term = jnp.where(at == n, prod, 0.0)
                totals[n] = term if totals[n] is None else totals[n] + term
        return totals

    totals = spread(both, wa, xbn, entries)
    for n in range(entries):
        sums_send[n // PAIR, (n % PAIR) * ROWS : (n % PAIR + 1) * ROWS] = totals[n]
    sum_copies = {}
    for i in sorted(range(owners), key=lambda i: -abs(offset(i))):
        for c in range(nsub):
            if i == zero_i:
                continue
            sum_copies[i, c] = pltpu.make_async_remote_copy(
                src_ref=sums_send.at[i],
                dst_ref=sums_recv.at[core, i],
                send_sem=sum_ssem.at[i, c],
                recv_sem=sum_rsem.at[core, i],
                device_id={"tile": tile_at(offset(i)), "sub": c},
                device_id_type=MESH,
            )
            sum_copies[i, c].start()
    self_copy = pltpu.make_async_remote_copy(
        src_ref=sums_send.at[zero_i],
        dst_ref=sums_recv.at[core, zero_i],
        send_sem=sum_ssem.at[zero_i, 0],
        recv_sem=sum_rsem.at[core, zero_i],
        device_id={"tile": me, "sub": other},
        device_id_type=MESH,
    )
    self_copy.start()
    for e in range(PAIR):
        sums_recv[core, zero_i, e * ROWS : (e + 1) * ROWS] = totals[PAIR * zero_i + e]

    heat = (1.0 - albedo) * sw + lw - 0.2 * sst - sens - lat
    fresh = pr - 0.5 * lat
    ocn_terms = jnp.concatenate([heat * wet, taux * wet, tauy * wet, fresh * wet, wet, pad], 0)
    ototals = spread(jnp.concatenate(split(ocn_terms), axis=0), wo, xbo, obl * nsub)
    own = []
    for m in range(obl):
        low, high = ototals[m], ototals[obl + m]
        oc_send[m] = jnp.where(core == 0, high, low)
        own.append(jnp.where(core == 0, low, high))
    ob_copy = pltpu.make_async_remote_copy(
        src_ref=oc_send,
        dst_ref=oc_recv,
        send_sem=ob_ssem,
        recv_sem=ob_rsem,
        device_id={"tile": me, "sub": other},
        device_id_type=MESH,
    )
    ob_copy.start()

    def recv_desc(src, dst, ssem, rsem):
        return pltpu.make_async_remote_copy(
            src_ref=src, dst_ref=dst, send_sem=ssem, recv_sem=rsem,
            device_id={"tile": me, "sub": other}, device_id_type=MESH,
        )

    for i in range(owners):
        desc = recv_desc(rows_send.at[0], rows_recv.at[i], row_ssem.at[0], row_rsem.at[i])
        if i == zero_i:
            @pl.when(core != zero_core)
            def _(desc=desc):
                desc.wait_recv()
        else:
            desc.wait_recv()
    width = owners * PAIR * ROWS
    places = jnp.concatenate([rows_recv[i] for i in range(owners)], axis=0)
    slot_of = lax.broadcasted_iota(jnp.int32, (owners, width), 1) // (PAIR * ROWS)
    mask = slot_of == lax.broadcasted_iota(jnp.int32, (owners, width), 0)
    place = jnp.sum(jnp.where(mask, places, 0), axis=0, keepdims=True)
    down = lax.broadcasted_iota(jnp.int32, (owned * ROWS, width), 0)
    across = lax.broadcasted_iota(jnp.int32, (owned * ROWS, width), 1)
    hit = down == place * ROWS + lax.rem(across, ROWS)
    landing = jnp.where(hit, 1.0, 0.0).astype(BF16)

    ob_copy.wait_recv()
    for m in range(obl):
        tot = own[m] + oc_recv[m]
        ocn_v[:, m * blk : (m + 1) * blk] = tot[:nflux] / jnp.maximum(tot[nflux : nflux + 1], 1.0)
    ocn_copy = pltpu.make_async_copy(ocn_v, ocn_out, out_sem.at[1])
    ocn_copy.start()

    for c in range(nsub):
        for i in range(owners):
            desc = recv_desc(sums_send.at[i], sums_recv.at[c, i], sum_ssem.at[i, 0], sum_rsem.at[c, i])
            if i == zero_i:
                @pl.when(core != c)
                def _(desc=desc):
                    desc.wait_recv()
            else:
                desc.wait_recv()
    arrived = sums_recv[0] + sums_recv[1]
    arrived = arrived.reshape(width, blk)
    high, low = split(arrived)
    final = jnp.dot(landing, high, preferred_element_type=F32) + jnp.dot(
        landing, low, preferred_element_type=F32
    )
    for a in range(owned):
        tot = final[a * ROWS : (a + 1) * ROWS]
        atm_v[:, a * blk : (a + 1) * blk] = tot[:nflux] / jnp.maximum(tot[nflux : nflux + 1], 1.0)
    atm_copy = pltpu.make_async_copy(atm_v, atm_out, out_sem.at[2])
    atm_copy.start()

    for k in range(half):
        if k == zero_i % half:
            @pl.when(core != zero_core)
            def _(k=k):
                pushes[k].wait_send()
        else:
            pushes[k].wait_send()
    for k in range(half):
        for c in range(nsub):
            copy = row_copies[k * nsub + c]
            if k == zero_i % half:
                @pl.when(jnp.logical_not(jnp.logical_and(core == zero_core, core == c)))
                def _(copy=copy):
                    copy.wait_send()
            else:
                copy.wait_send()
    oc_copy.wait_send()
    pick_copy.wait_send()
    for copy in sum_copies.values():
        copy.wait_send()
    self_copy.wait_send()
    ob_copy.wait_send()
    ocn_copy.wait()
    atm_copy.wait()


def solution(mesh):
    ntile, nsub = mesh.shape["tile"], mesh.shape["sub"]

    def per_device(
        atm_state, ocn_state, need_atm, xb_need, xb_ocn, xb_count, sea_mask, cell_area, w_atm, w_ocn
    ):
        nb, blk, _ = w_atm.shape
        nflux = 4
        mine = need_atm.shape[0]
        half = mine // PAIR
        owners = half * nsub
        entries = mine * nsub
        fields_a, acells = atm_state.shape
        fields_o, ocells = ocn_state.shape
        obl = ocells // blk
        owned = acells // blk
        cells = nb * blk
        dma = pltpu.SemaphoreType.DMA
        return pl.pallas_call(
            functools.partial(kernel, ntile, nsub, blk),
            out_shape=(
                jax.ShapeDtypeStruct((nflux, acells), F32),
                jax.ShapeDtypeStruct((nflux, ocells), F32),
            ),
            in_specs=[pl.BlockSpec(memory_space=pl.ANY)] * 10,
            out_specs=(pl.BlockSpec(memory_space=pl.ANY),) * 2,
            scratch_shapes=[
                pltpu.VMEM((owned, fields_a, blk), BF16),
                pltpu.VMEM((nsub, obl, fields_o, blk), BF16),
                pltpu.SMEM((mine,), jnp.int32),
                pltpu.SMEM((nb,), jnp.int32),
                pltpu.SMEM((nb,), jnp.int32),
                pltpu.SMEM((1,), jnp.int32),
                pltpu.VMEM((1, cells), jnp.int32),
                pltpu.VMEM((1, cells), F32),
                pltpu.VMEM((nb, blk, blk), BF16),
                pltpu.VMEM((nb, blk, blk), BF16),
                pltpu.VMEM((half, owned, fields_a, blk), BF16),
                pltpu.VMEM((entries, fields_a, blk), BF16),
                pltpu.VMEM((half, 1, blk), jnp.int32),
                pltpu.VMEM((owners, 1, blk), jnp.int32),
                pltpu.VMEM((owners, PAIR * ROWS, blk), F32),
                pltpu.VMEM((nsub, owners, PAIR * ROWS, blk), F32),
                pltpu.VMEM((obl, ROWS, blk), F32),
                pltpu.VMEM((obl, ROWS, blk), F32),
                pltpu.VMEM((nflux, acells), F32),
                pltpu.VMEM((nflux, ocells), F32),
                dma((8,)),
                dma((owned + obl,)),
                dma((half,)),
                dma((half,)),
                dma((half * nsub,)),
                dma((owners,)),
                dma(()),
                dma(()),
                dma(()),
                dma(()),
                dma((owners, nsub)),
                dma((nsub, owners)),
                dma(()),
                dma(()),
                dma((3,)),
            ],
            compiler_params=pltpu.CompilerParams(collective_id=0, has_side_effects=True),
        )(
            atm_state, ocn_state, need_atm, xb_need, xb_ocn, xb_count,
            sea_mask.reshape(1, cells), cell_area.reshape(1, cells), w_atm, w_ocn,
        )

    spread_all = P(("tile", "sub"))
    weights = P(("tile", "sub"), None, None)
    return jax.shard_map(
        per_device,
        mesh=mesh,
        in_specs=(
            P(None, ("member", "tile")),
            P(None, ("member", "tile", "sub")),
            spread_all, spread_all, spread_all, spread_all, spread_all, spread_all,
            weights, weights,
        ),
        out_specs=(P(None, ("member", "tile")), P(None, ("member", "tile", "sub"))),
        check_vma=False,
    )
```

```python
import functools

import jax
import jax.numpy as jnp
from jax import lax
from jax.experimental import pallas as pl
from jax.experimental.pallas import tpu as pltpu
from jax.sharding import PartitionSpec as P

MESH = pl.DeviceIdType.MESH
ROWS = 8
PAIR = 2
F32 = jnp.float32
BF16 = jnp.bfloat16
TRANSPOSED = (((1,), (1,)), ((), ()))


def split(value):
    high = value.astype(BF16)
    low = (value - high.astype(F32)).astype(BF16)
    return high, low


def kernel(
    ntile, nsub, blk,
    state_hbm, ocean_hbm, need_hbm, xbn_hbm, xbo_hbm, count_hbm, sea_hbm, area_hbm, wa_hbm, wo_hbm,
    atm_out, ocn_out,
    state, octab, need, xbn, xbo, count, sea, area, wa, wo,
    table, picked, rows_send, rows_recv, area_send, area_recv, sums_send, sums_recv, oc_send, oc_recv,
    load_sem, block_sem, push_ssem, push_rsem, row_ssem, row_rsem, oc_ssem, oc_rsem,
    pick_ssem, pick_rsem, area_ssem, area_rsem, sum_ssem, sum_rsem, ob_ssem, ob_rsem, keep_sem,
):
    me = lax.axis_index("tile")
    core = lax.axis_index("sub")
    other = 1 - core
    nb = wa.shape[0]
    mine = need.shape[0]
    half = mine // PAIR
    owners = half * nsub
    entries = mine * nsub
    owned = state.shape[0]
    obl = octab.shape[1]
    nflux = atm_out.shape[0]
    flux_lanes = owners * PAIR * nflux

    def offset(i):
        return ntile // 2 if i == owners - 1 else i - owners // 2 + 1

    def tile_at(delta):
        return lax.rem(me + delta + ntile, ntile)

    zero_i = [i for i in range(owners) if offset(i) == 0][0]

    local = [
        pltpu.make_async_copy(src, dst, load_sem.at[k])
        for k, (src, dst) in enumerate(
            [
                (need_hbm, need),
                (wo_hbm, wo),
                (wa_hbm, wa),
                (xbo_hbm, xbo),
                (xbn_hbm, xbn),
                (count_hbm, count),
                (sea_hbm, sea),
                (area_hbm, area),
            ]
        )
    ]
    blocks = [
        pltpu.make_async_copy(
            state_hbm.at[:, pl.ds(n * blk, blk)], state.at[n], block_sem.at[n]
        )
        for n in range(owned)
    ] + [
        pltpu.make_async_copy(
            ocean_hbm.at[:, pl.ds(n * blk, blk)], octab.at[core, n], block_sem.at[owned + n]
        )
        for n in range(obl)
    ]
    for copy in blocks + local:
        copy.start()

    barrier = pltpu.get_barrier_semaphore()
    for i in range(owners):
        for c in range(nsub):
            if i == zero_i:
                continue
            pl.semaphore_signal(
                barrier, inc=1, device_id={"tile": tile_at(offset(i)), "sub": c}, device_id_type=MESH
            )
    pl.semaphore_signal(barrier, inc=1, device_id={"tile": me, "sub": other}, device_id_type=MESH)

    local[0].wait()
    lane = lax.broadcasted_iota(jnp.int32, (1, blk), 1)
    odd = jnp.where(lane < flux_lanes, lax.rem(lane // nflux, PAIR), lax.rem(lane, PAIR))
    for k in range(half):
        first = lax.rem(need[PAIR * k], owned)
        second = lax.rem(need[PAIR * k + 1], owned)
        rows_send[k] = jnp.where(odd == 0, first, second)
    for copy in blocks:
        copy.wait()
    pl.semaphore_wait(barrier, owners * nsub - 1)

    def delta_of(k):
        out = jnp.int32(0)
        for c in range(nsub):
            out = jnp.where(core == c, jnp.int32(offset(c * half + k)), out)
        return out

    deltas = [delta_of(k) for k in range(half)]
    pushes = [
        pltpu.make_async_remote_copy(
            src_ref=state,
            dst_ref=table.at[k],
            send_sem=push_ssem.at[k],
            recv_sem=push_rsem.at[k],
            device_id={"tile": tile_at(-deltas[k]), "sub": core},
            device_id_type=MESH,
        )
        for k in range(half)
    ]
    keep = pltpu.make_async_copy(state, table.at[zero_i % half], keep_sem)
    zero_core = zero_i // half
    order = sorted(range(half), key=lambda k: -abs(offset(k)))
    for k in order:
        if k == zero_i % half:
            @pl.when(core == zero_core)
            def _():
                keep.start()

            @pl.when(core != zero_core)
            def _(k=k):
                pushes[k].start()
        else:
            pushes[k].start()
    oc_copy = pltpu.make_async_remote_copy(
        src_ref=octab.at[core],
        dst_ref=octab.at[core],
        send_sem=oc_ssem,
        recv_sem=oc_rsem,
        device_id={"tile": me, "sub": other},
        device_id_type=MESH,
    )
    oc_copy.start()

    row_copies = []
    for k in range(half):
        slot = core * half + k
        for c in range(nsub):
            row_copies.append(
                pltpu.make_async_remote_copy(
                    src_ref=rows_send.at[k],
                    dst_ref=rows_recv.at[slot],
                    send_sem=row_ssem.at[k * nsub + c],
                    recv_sem=row_rsem.at[slot],
                    device_id={"tile": tile_at(deltas[k]), "sub": c},
                    device_id_type=MESH,
                )
            )
            copy = row_copies[-1]
            if k == zero_i % half:
                here = jnp.logical_and(core == zero_core, core == c)

                @pl.when(here)
                def _(k=k):
                    rows_recv[zero_i] = rows_send[k]

                @pl.when(jnp.logical_not(here))
                def _(copy=copy):
                    copy.start()
            else:
                copy.start()

    ones = jnp.ones((ROWS, blk), BF16)
    local[1].wait()
    local[3].wait()
    oc_copy.wait_recv()
    oxs = []
    for b in range(nb):
        m = xbo[b]
        cells = octab[lax.div(m, obl), lax.rem(m, obl)]
        w = wo[b]
        top = lax.dot_general(cells, w, TRANSPOSED, preferred_element_type=F32)
        den = lax.dot_general(ones, w, TRANSPOSED, preferred_element_type=F32)
        oxs.append(top / den[: top.shape[0]])
    ox = jnp.concatenate(oxs, axis=1)
    sst, uo, vo, oa = [ox[f : f + 1] for f in range(4)]
    albedo = 0.06 + 0.05 * (1.0 + jnp.tanh(0.5 * oa))
    local[2].wait()
    dens = jnp.concatenate(
        [lax.dot_general(ones, wa[b], TRANSPOSED, preferred_element_type=F32) for b in range(nb)],
        axis=1,
    )
    rden = 1.0 / dens
    for k in (4, 5, 6, 7):
        local[k].wait()
    cell = lax.broadcasted_iota(jnp.int32, (1, nb * blk), 1)
    weighted = jnp.where(cell < count[0] * blk, area[...], 0.0)
    wet = weighted * sea[...].astype(F32)

    def spread(both, w, index, number, step, shift):
        totals = [None] * number
        for b in range(nb):
            prod = jnp.dot(both[:, b * blk : (b + 1) * blk], w[b], preferred_element_type=F32)
            prod = prod[:ROWS] + prod[ROWS:]
            at = index[b] - shift
            for n in range(number):
                term = jnp.where(at == n * step, prod, 0.0)
                totals[n] = term if totals[n] is None else totals[n] + term
        return totals

    def send_owners(src, dst, ssem, rsem):
        copies = []
        for i in sorted(range(owners), key=lambda i: -abs(offset(i))):
            for c in range(nsub):
                if i == zero_i and c > 0:
                    continue
                copy = pltpu.make_async_remote_copy(
                    src_ref=src.at[i],
                    dst_ref=dst.at[core, i],
                    send_sem=ssem.at[i, c],
                    recv_sem=rsem.at[core, i],
                    device_id={"tile": tile_at(offset(i)), "sub": other if i == zero_i else c},
                    device_id_type=MESH,
                )
                copy.start()
                copies.append(copy)
        return copies

    row_id = lax.broadcasted_iota(jnp.int32, (ROWS, blk), 0)
    areas = jnp.concatenate(split(jnp.broadcast_to(weighted, (ROWS, nb * blk))), axis=0)
    totals = spread(areas, wa, xbn, owners, PAIR, lax.rem(row_id, PAIR))
    for i in range(owners):
        area_send[i] = totals[i][:PAIR]
    area_recv[core, zero_i] = totals[zero_i][:PAIR]

    for k in range(half):
        if k == zero_i % half:
            @pl.when(core == zero_core)
            def _():
                keep.wait()

            @pl.when(core != zero_core)
            def _(k=k):
                pushes[k].wait_recv()
        else:
            pushes[k].wait_recv()
    for e in range(mine):
        picked[core * mine + e] = table[e // PAIR, lax.rem(need[e], owned)]
    part = picked.at[pl.ds(core * mine, mine)]
    pick_copy = pltpu.make_async_remote_copy(
        src_ref=part,
        dst_ref=part,
        send_sem=pick_ssem,
        recv_sem=pick_rsem,
        device_id={"tile": me, "sub": other},
        device_id_type=MESH,
    )
    pick_copy.start()
    area_copies = send_owners(area_send, area_recv, area_ssem, area_rsem)
    pick_copy.wait_recv()
    ax = jnp.concatenate(
        [
            lax.dot_general(picked[xbn[b]], wa[b], TRANSPOSED, preferred_element_type=F32)
            for b in range(nb)
        ],
        axis=1,
    )
    ax = ax * rden
    ta, qa, ua, va, ps, sw, lw, pr = [ax[f : f + 1] for f in range(8)]

    du = ua - uo
    dv = va - vo
    speed = jnp.sqrt(du * du + dv * dv + 1.0)
    cd = (0.3 + 0.1 * jnp.tanh(ps)) * speed
    sens = cd * (sst - ta)
    lat = cd * (0.5 * sst - qa)
    taux = cd * du
    tauy = cd * dv
    pad = jnp.zeros((ROWS - 5, nb * blk), F32)
    fluxes = [sens * wet, lat * wet, taux * wet, tauy * wet]
    both = jnp.concatenate(split(jnp.concatenate(fluxes * PAIR, axis=0)), axis=0)
    totals = spread(both, wa, xbn, owners, PAIR, row_id // nflux)
    for i in range(owners):
        sums_send[i] = totals[i]
    sum_copies = send_owners(sums_send, sums_recv, sum_ssem, sum_rsem)
    sums_recv[core, zero_i] = totals[zero_i]

    heat = (1.0 - albedo) * sw + lw - 0.2 * sst - sens - lat
    fresh = pr - 0.5 * lat
    pad = jnp.zeros((ROWS - nflux - 1, nb * blk), F32)
    ocn_terms = jnp.concatenate([heat * wet, taux * wet, tauy * wet, fresh * wet, wet, pad], 0)
    ototals = spread(jnp.concatenate(split(ocn_terms), axis=0), wo, xbo, obl * nsub, 1, 0)
    own = []
    for m in range(obl):
        low, high = ototals[m], ototals[obl + m]
        oc_send[m] = jnp.where(core == 0, high, low)
        own.append(jnp.where(core == 0, low, high))
    ob_copy = pltpu.make_async_remote_copy(
        src_ref=oc_send,
        dst_ref=oc_recv,
        send_sem=ob_ssem,
        recv_sem=ob_rsem,
        device_id={"tile": me, "sub": other},
        device_id_type=MESH,
    )
    ob_copy.start()

    def recv_desc(src, dst, ssem, rsem):
        return pltpu.make_async_remote_copy(
            src_ref=src, dst_ref=dst, send_sem=ssem, recv_sem=rsem,
            device_id={"tile": me, "sub": other}, device_id_type=MESH,
        )

    for i in range(owners):
        desc = recv_desc(rows_send.at[0], rows_recv.at[i], row_ssem.at[0], row_rsem.at[i])
        if i == zero_i:
            @pl.when(core != zero_core)
            def _(desc=desc):
                desc.wait_recv()
        else:
            desc.wait_recv()
    places = jnp.concatenate([rows_recv[i] for i in range(owners)], axis=0)
    lanes = lax.broadcasted_iota(jnp.int32, (owners, blk), 1)
    slot_of = jnp.where(
        lanes < flux_lanes, lanes // (PAIR * nflux), (lanes - flux_lanes) // PAIR
    )
    mask = slot_of == lax.broadcasted_iota(jnp.int32, (owners, blk), 0)
    place = jnp.sum(jnp.where(mask, places, 0), axis=0, keepdims=True)
    down = lax.broadcasted_iota(jnp.int32, (owned * nflux, blk), 0)
    across = lax.broadcasted_iota(jnp.int32, (owned * nflux, blk), 1)
    hit = jnp.logical_and(
        down // nflux == place,
        jnp.logical_or(across >= flux_lanes, lax.rem(down, nflux) == lax.rem(across, nflux)),
    )
    landing = jnp.where(hit, 1.0, 0.0)
    landing_flux = landing[:, :flux_lanes].astype(BF16)
    landing_area = landing[:, flux_lanes : flux_lanes + owners * PAIR].astype(BF16)

    def land(landing, value):
        high, low = split(value)
        return jnp.dot(landing, high, preferred_element_type=F32) + jnp.dot(
            landing, low, preferred_element_type=F32
        )

    def wait_owners(src, dst, ssem, rsem):
        for c in range(nsub):
            for i in range(owners):
                desc = recv_desc(src.at[i], dst.at[c, i], ssem.at[i, 0], rsem.at[c, i])
                if i == zero_i:
                    @pl.when(core != c)
                    def _(desc=desc):
                        desc.wait_recv()
                else:
                    desc.wait_recv()

    ob_copy.wait_recv()
    for m in range(obl):
        tot = own[m] + oc_recv[m]
        ocn_out[:, m * blk : (m + 1) * blk] = tot[:nflux] / jnp.maximum(tot[nflux : nflux + 1], 1.0)

    wait_owners(area_send, area_recv, area_ssem, area_rsem)
    arrived = jnp.concatenate([area_recv[0, i] + area_recv[1, i] for i in range(owners)], axis=0)
    scale = 1.0 / jnp.maximum(land(landing_area, arrived), 1.0)

    wait_owners(sums_send, sums_recv, sum_ssem, sum_rsem)
    arrived = (sums_recv[0] + sums_recv[1]).reshape(flux_lanes, blk)
    final = land(landing_flux, arrived) * scale
    for a in range(owned):
        atm_out[:, a * blk : (a + 1) * blk] = final[a * nflux : (a + 1) * nflux]

    for k in range(half):
        if k == zero_i % half:
            @pl.when(core != zero_core)
            def _(k=k):
                pushes[k].wait_send()
        else:
            pushes[k].wait_send()
    for k in range(half):
        for c in range(nsub):
            copy = row_copies[k * nsub + c]
            if k == zero_i % half:
                @pl.when(jnp.logical_not(jnp.logical_and(core == zero_core, core == c)))
                def _(copy=copy):
                    copy.wait_send()
            else:
                copy.wait_send()
    oc_copy.wait_send()
    pick_copy.wait_send()
    for copy in area_copies + sum_copies:
        copy.wait_send()
    ob_copy.wait_send()


def solution(mesh):
    ntile, nsub = mesh.shape["tile"], mesh.shape["sub"]

    def per_device(
        atm_state, ocn_state, need_atm, xb_need, xb_ocn, xb_count, sea_mask, cell_area, w_atm, w_ocn
    ):
        nb, blk, _ = w_atm.shape
        nflux = 4
        mine = need_atm.shape[0]
        half = mine // PAIR
        owners = half * nsub
        entries = mine * nsub
        fields_a, acells = atm_state.shape
        fields_o, ocells = ocn_state.shape
        obl = ocells // blk
        owned = acells // blk
        cells = nb * blk
        dma = pltpu.SemaphoreType.DMA
        return pl.pallas_call(
            functools.partial(kernel, ntile, nsub, blk),
            out_shape=(
                pltpu.VMEM((nflux, acells), F32),
                pltpu.VMEM((nflux, ocells), F32),
            ),
            in_specs=[pl.BlockSpec(memory_space=pltpu.HBM)] * 10,
            out_specs=(pl.BlockSpec(memory_space=pltpu.VMEM),) * 2,
            scratch_shapes=[
                pltpu.VMEM((owned, fields_a, blk), BF16),
                pltpu.VMEM((nsub, obl, fields_o, blk), BF16),
                pltpu.SMEM((mine,), jnp.int32),
                pltpu.SMEM((nb,), jnp.int32),
                pltpu.SMEM((nb,), jnp.int32),
                pltpu.SMEM((1,), jnp.int32),
                pltpu.VMEM((1, cells), jnp.int32),
                pltpu.VMEM((1, cells), F32),
                pltpu.VMEM((nb, blk, blk), BF16),
                pltpu.VMEM((nb, blk, blk), BF16),
                pltpu.VMEM((half, owned, fields_a, blk), BF16),
                pltpu.VMEM((entries, fields_a, blk), BF16),
                pltpu.VMEM((half, 1, blk), jnp.int32),
                pltpu.VMEM((owners, 1, blk), jnp.int32),
                pltpu.VMEM((owners, PAIR, blk), F32),
                pltpu.VMEM((nsub, owners, PAIR, blk), F32),
                pltpu.VMEM((owners, PAIR * nflux, blk), F32),
                pltpu.VMEM((nsub, owners, PAIR * nflux, blk), F32),
                pltpu.VMEM((obl, ROWS, blk), F32),
                pltpu.VMEM((obl, ROWS, blk), F32),
                dma((8,)),
                dma((owned + obl,)),
                dma((half,)),
                dma((half,)),
                dma((half * nsub,)),
                dma((owners,)),
                dma(()),
                dma(()),
                dma(()),
                dma(()),
                dma((owners, nsub)),
                dma((nsub, owners)),
                dma((owners, nsub)),
                dma((nsub, owners)),
                dma(()),
                dma(()),
                dma(()),
            ],
            compiler_params=pltpu.CompilerParams(collective_id=0, has_side_effects=True),
        )(
            atm_state, ocn_state, need_atm, xb_need, xb_ocn, xb_count,
            sea_mask.reshape(1, cells), cell_area.reshape(1, cells), w_atm, w_ocn,
        )

    spread_all = P(("tile", "sub"))
    weights = P(("tile", "sub"), None, None)
    return jax.shard_map(
        per_device,
        mesh=mesh,
        in_specs=(
            P(None, ("member", "tile")),
            P(None, ("member", "tile", "sub")),
            spread_all, spread_all, spread_all, spread_all, spread_all, spread_all,
            weights, weights,
        ),
        out_specs=(P(None, ("member", "tile")), P(None, ("member", "tile", "sub"))),
        check_vma=False,
    )
```

```python
import functools

import jax
import jax.numpy as jnp
from jax import lax
from jax.experimental import pallas as pl
from jax.experimental.pallas import tpu as pltpu
from jax.sharding import PartitionSpec as P

MESH = pl.DeviceIdType.MESH
ROWS = 8
PAIR = 2
F32 = jnp.float32
BF16 = jnp.bfloat16
TRANSPOSED = (((1,), (1,)), ((), ()))


def split(value):
    high = value.astype(BF16)
    low = (value - high.astype(F32)).astype(BF16)
    return high, low


def kernel(
    ntile, nsub, blk,
    state_hbm, ocean_hbm, need_hbm, xbn_hbm, xbo_hbm, count_hbm, sea_hbm, area_hbm, wa_hbm, wo_hbm,
    atm_out, ocn_out,
    state, octab, need, xbn, xbo, count, sea, area, wa, wo,
    table, picked, rows_send, rows_recv, area_send, area_recv, sums_send, sums_recv, oc_send, oc_recv,
    load_sem, block_sem, push_ssem, push_rsem, row_ssem, row_rsem, oc_ssem, oc_rsem,
    pick_ssem, pick_rsem, area_ssem, area_rsem, sum_ssem, sum_rsem, ob_ssem, ob_rsem, keep_sem,
):
    me = lax.axis_index("tile")
    core = lax.axis_index("sub")
    other = 1 - core
    nb = wa.shape[0]
    mine = need.shape[0]
    half = mine // PAIR
    owners = half * nsub
    entries = mine * nsub
    owned = state.shape[0]
    obl = octab.shape[1]
    nflux = atm_out.shape[0]
    flux_lanes = owners * PAIR * nflux

    def offset(i):
        return ntile // 2 if i == owners - 1 else i - owners // 2 + 1

    def tile_at(delta):
        return lax.rem(me + delta + ntile, ntile)

    zero_i = [i for i in range(owners) if offset(i) == 0][0]

    local = [
        pltpu.make_async_copy(src, dst, load_sem.at[k])
        for k, (src, dst) in enumerate(
            [
                (need_hbm, need),
                (wo_hbm, wo),
                (wa_hbm, wa),
                (xbo_hbm, xbo),
                (xbn_hbm, xbn),
                (count_hbm, count),
                (sea_hbm, sea),
                (area_hbm, area),
            ]
        )
    ]
    blocks = [
        pltpu.make_async_copy(
            state_hbm.at[:, pl.ds(n * blk, blk)], state.at[n], block_sem.at[n]
        )
        for n in range(owned)
    ] + [
        pltpu.make_async_copy(
            ocean_hbm.at[:, pl.ds(n * blk, blk)], octab.at[core, n], block_sem.at[owned + n]
        )
        for n in range(obl)
    ]
    for copy in blocks + local:
        copy.start()

    barrier = pltpu.get_barrier_semaphore()
    for i in range(owners):
        for c in range(nsub):
            if i == zero_i:
                continue
            pl.semaphore_signal(
                barrier, inc=1, device_id={"tile": tile_at(offset(i)), "sub": c}, device_id_type=MESH
            )
    pl.semaphore_signal(barrier, inc=1, device_id={"tile": me, "sub": other}, device_id_type=MESH)

    local[0].wait()
    lane = lax.broadcasted_iota(jnp.int32, (1, blk), 1)
    odd = jnp.where(lane < flux_lanes, lax.rem(lane // nflux, PAIR), lax.rem(lane, PAIR))
    for k in range(half):
        first = lax.rem(need[PAIR * k], owned)
        second = lax.rem(need[PAIR * k + 1], owned)
        rows_send[k] = jnp.where(odd == 0, first, second)
    for copy in blocks:
        copy.wait()
    pl.semaphore_wait(barrier, owners * nsub - 1)

    def delta_of(k):
        out = jnp.int32(0)
        for c in range(nsub):
            out = jnp.where(core == c, jnp.int32(offset(c * half + k)), out)
        return out

    deltas = [delta_of(k) for k in range(half)]
    pushes = [
        pltpu.make_async_remote_copy(
            src_ref=state,
            dst_ref=table.at[k],
            send_sem=push_ssem.at[k],
            recv_sem=push_rsem.at[k],
            device_id={"tile": tile_at(-deltas[k]), "sub": core},
            device_id_type=MESH,
        )
        for k in range(half)
    ]
    keep = pltpu.make_async_copy(state, table.at[zero_i % half], keep_sem)
    zero_core = zero_i // half
    order = sorted(range(half), key=lambda k: -abs(offset(k)))
    for k in order:
        if k == zero_i % half:
            @pl.when(core == zero_core)
            def _():
                keep.start()

            @pl.when(core != zero_core)
            def _(k=k):
                pushes[k].start()
        else:
            pushes[k].start()
    oc_copy = pltpu.make_async_remote_copy(
        src_ref=octab.at[core],
        dst_ref=octab.at[core],
        send_sem=oc_ssem,
        recv_sem=oc_rsem,
        device_id={"tile": me, "sub": other},
        device_id_type=MESH,
    )
    oc_copy.start()

    row_copies = []
    for k in range(half):
        slot = core * half + k
        for c in range(nsub):
            row_copies.append(
                pltpu.make_async_remote_copy(
                    src_ref=rows_send.at[k],
                    dst_ref=rows_recv.at[slot],
                    send_sem=row_ssem.at[k * nsub + c],
                    recv_sem=row_rsem.at[slot],
                    device_id={"tile": tile_at(deltas[k]), "sub": c},
                    device_id_type=MESH,
                )
            )
            copy = row_copies[-1]
            if k == zero_i % half:
                here = jnp.logical_and(core == zero_core, core == c)

                @pl.when(here)
                def _(k=k):
                    rows_recv[zero_i] = rows_send[k]

                @pl.when(jnp.logical_not(here))
                def _(copy=copy):
                    copy.start()
            else:
                copy.start()

    ones = jnp.ones((ROWS, blk), BF16)
    local[1].wait()
    local[3].wait()
    oc_copy.wait_recv()
    oxs = []
    for b in range(nb):
        m = xbo[b]
        cells = octab[lax.div(m, obl), lax.rem(m, obl)]
        w = wo[b]
        top = lax.dot_general(cells, w, TRANSPOSED, preferred_element_type=F32)
        den = lax.dot_general(ones, w, TRANSPOSED, preferred_element_type=F32)
        oxs.append(top / den[: top.shape[0]])
    ox = jnp.concatenate(oxs, axis=1)
    sst, uo, vo, oa = [ox[f : f + 1] for f in range(4)]
    albedo = 0.06 + 0.05 * (1.0 + jnp.tanh(0.5 * oa))
    local[2].wait()
    dens = jnp.concatenate(
        [lax.dot_general(ones, wa[b], TRANSPOSED, preferred_element_type=F32) for b in range(nb)],
        axis=1,
    )
    rden = 1.0 / dens
    for k in (4, 5, 6, 7):
        local[k].wait()
    cell = lax.broadcasted_iota(jnp.int32, (1, nb * blk), 1)
    weighted = jnp.where(cell < count[0] * blk, area[...], 0.0)
    wet = weighted * sea[...].astype(F32)

    def spread(both, w, index, number, step, shift):
        totals = [None] * number
        for b in range(nb):
            prod = jnp.dot(both[:, b * blk : (b + 1) * blk], w[b], preferred_element_type=F32)
            prod = prod[:ROWS] + prod[ROWS:]
            at = index[b] - shift
            for n in range(number):
                term = jnp.where(at == n * step, prod, 0.0)
                totals[n] = term if totals[n] is None else totals[n] + term
        return totals

    def send_owners(src, dst, ssem, rsem):
        copies = []
        for i in sorted(range(owners), key=lambda i: -abs(offset(i))):
            for c in range(nsub):
                if i == zero_i and c > 0:
                    continue
                copy = pltpu.make_async_remote_copy(
                    src_ref=src.at[i],
                    dst_ref=dst.at[core, i],
                    send_sem=ssem.at[i, c],
                    recv_sem=rsem.at[core, i],
                    device_id={"tile": tile_at(offset(i)), "sub": other if i == zero_i else c},
                    device_id_type=MESH,
                )
                copy.start()
                copies.append(copy)
        return copies

    row_id = lax.broadcasted_iota(jnp.int32, (ROWS, blk), 0)
    areas = jnp.concatenate(split(jnp.broadcast_to(weighted, (ROWS, nb * blk))), axis=0)
    totals = spread(areas, wa, xbn, owners, PAIR, lax.rem(row_id, PAIR))
    for i in range(owners):
        area_send[i] = totals[i][:PAIR]
    area_recv[core, zero_i] = totals[zero_i][:PAIR]

    for k in range(half):
        if k == zero_i % half:
            @pl.when(core == zero_core)
            def _():
                keep.wait()

            @pl.when(core != zero_core)
            def _(k=k):
                pushes[k].wait_recv()
        else:
            pushes[k].wait_recv()
    for e in range(mine):
        picked[core * mine + e] = table[e // PAIR, lax.rem(need[e], owned)]
    part = picked.at[pl.ds(core * mine, mine)]
    pick_copy = pltpu.make_async_remote_copy(
        src_ref=part,
        dst_ref=part,
        send_sem=pick_ssem,
        recv_sem=pick_rsem,
        device_id={"tile": me, "sub": other},
        device_id_type=MESH,
    )
    pick_copy.start()
    area_copies = send_owners(area_send, area_recv, area_ssem, area_rsem)
    pick_copy.wait_recv()
    ax = jnp.concatenate(
        [
            lax.dot_general(picked[xbn[b]], wa[b], TRANSPOSED, preferred_element_type=F32)
            for b in range(nb)
        ],
        axis=1,
    )
    ax = ax * rden
    ta, qa, ua, va, ps, sw, lw, pr = [ax[f : f + 1] for f in range(8)]

    du = ua - uo
    dv = va - vo
    speed = jnp.sqrt(du * du + dv * dv + 1.0)
    cd = (0.3 + 0.1 * jnp.tanh(ps)) * speed
    sens = cd * (sst - ta)
    lat = cd * (0.5 * sst - qa)
    taux = cd * du
    tauy = cd * dv
    pad = jnp.zeros((ROWS - 5, nb * blk), F32)
    fluxes = [sens * wet, lat * wet, taux * wet, tauy * wet]
    both = jnp.concatenate(split(jnp.concatenate(fluxes * PAIR, axis=0)), axis=0)
    totals = spread(both, wa, xbn, owners, PAIR, row_id // nflux)
    for i in range(owners):
        sums_send[i] = totals[i]
    sum_copies = send_owners(sums_send, sums_recv, sum_ssem, sum_rsem)
    sums_recv[core, zero_i] = totals[zero_i]

    heat = (1.0 - albedo) * sw + lw - 0.2 * sst - sens - lat
    fresh = pr - 0.5 * lat
    pad = jnp.zeros((ROWS - nflux - 1, nb * blk), F32)
    ocn_terms = jnp.concatenate([heat * wet, taux * wet, tauy * wet, fresh * wet, wet, pad], 0)
    ototals = spread(jnp.concatenate(split(ocn_terms), axis=0), wo, xbo, obl * nsub, 1, 0)
    own = []
    for m in range(obl):
        low, high = ototals[m], ototals[obl + m]
        oc_send[m] = jnp.where(core == 0, high, low)
        own.append(jnp.where(core == 0, low, high))
    ob_copy = pltpu.make_async_remote_copy(
        src_ref=oc_send,
        dst_ref=oc_recv,
        send_sem=ob_ssem,
        recv_sem=ob_rsem,
        device_id={"tile": me, "sub": other},
        device_id_type=MESH,
    )
    ob_copy.start()

    def recv_desc(src, dst, ssem, rsem):
        return pltpu.make_async_remote_copy(
            src_ref=src, dst_ref=dst, send_sem=ssem, recv_sem=rsem,
            device_id={"tile": me, "sub": other}, device_id_type=MESH,
        )

    for i in range(owners):
        desc = recv_desc(rows_send.at[0], rows_recv.at[i], row_ssem.at[0], row_rsem.at[i])
        if i == zero_i:
            @pl.when(core != zero_core)
            def _(desc=desc):
                desc.wait_recv()
        else:
            desc.wait_recv()
    places = jnp.concatenate([rows_recv[i] for i in range(owners)], axis=0)
    lanes = lax.broadcasted_iota(jnp.int32, (owners, blk), 1)
    slot_of = jnp.where(
        lanes < flux_lanes, lanes // (PAIR * nflux), (lanes - flux_lanes) // PAIR
    )
    mask = slot_of == lax.broadcasted_iota(jnp.int32, (owners, blk), 0)
    place = jnp.sum(jnp.where(mask, places, 0), axis=0, keepdims=True)
    down = lax.broadcasted_iota(jnp.int32, (owned * nflux, blk), 0)
    across = lax.broadcasted_iota(jnp.int32, (owned * nflux, blk), 1)
    hit = jnp.logical_and(
        down // nflux == place,
        jnp.logical_or(across >= flux_lanes, lax.rem(down, nflux) == lax.rem(across, nflux)),
    )
    landing = jnp.where(hit, 1.0, 0.0)
    landing_flux = landing[:, :flux_lanes].astype(BF16)
    landing_area = landing[:, flux_lanes : flux_lanes + owners * PAIR].astype(BF16)

    def land(landing, value):
        high, low = split(value)
        return jnp.dot(landing, high, preferred_element_type=F32) + jnp.dot(
            landing, low, preferred_element_type=F32
        )

    def wait_owners(src, dst, ssem, rsem):
        for c in range(nsub):
            for i in range(owners):
                desc = recv_desc(src.at[i], dst.at[c, i], ssem.at[i, 0], rsem.at[c, i])
                if i == zero_i:
                    @pl.when(core != c)
                    def _(desc=desc):
                        desc.wait_recv()
                else:
                    desc.wait_recv()

    ob_copy.wait_recv()
    for m in range(obl):
        tot = own[m] + oc_recv[m]
        ocn_out[:, m * blk : (m + 1) * blk] = tot[:nflux] / jnp.maximum(tot[nflux : nflux + 1], 1.0)

    wait_owners(area_send, area_recv, area_ssem, area_rsem)
    arrived = jnp.concatenate([area_recv[0, i] + area_recv[1, i] for i in range(owners)], axis=0)
    scale = 1.0 / jnp.maximum(land(landing_area, arrived), 1.0)

    wait_owners(sums_send, sums_recv, sum_ssem, sum_rsem)
    arrived = (sums_recv[0] + sums_recv[1]).reshape(flux_lanes, blk)
    final = land(landing_flux, arrived) * scale
    for a in range(owned):
        atm_out[:, a * blk : (a + 1) * blk] = final[a * nflux : (a + 1) * nflux]

    for k in range(half):
        if k == zero_i % half:
            @pl.when(core != zero_core)
            def _(k=k):
                pushes[k].wait_send()
        else:
            pushes[k].wait_send()
    for k in range(half):
        for c in range(nsub):
            copy = row_copies[k * nsub + c]
            if k == zero_i % half:
                @pl.when(jnp.logical_not(jnp.logical_and(core == zero_core, core == c)))
                def _(copy=copy):
                    copy.wait_send()
            else:
                copy.wait_send()
    oc_copy.wait_send()
    pick_copy.wait_send()
    for copy in area_copies + sum_copies:
        copy.wait_send()
    ob_copy.wait_send()


def write_out(atm, ocn, atm_hbm, ocn_hbm, sem):
    copies = [
        pltpu.make_async_copy(src, dst, sem.at[k])
        for k, (src, dst) in enumerate([(atm, atm_hbm), (ocn, ocn_hbm)])
    ]
    for copy in copies:
        copy.start()
    for copy in copies:
        copy.wait()


def solution(mesh):
    ntile, nsub = mesh.shape["tile"], mesh.shape["sub"]

    def per_device(
        atm_state, ocn_state, need_atm, xb_need, xb_ocn, xb_count, sea_mask, cell_area, w_atm, w_ocn
    ):
        nb, blk, _ = w_atm.shape
        nflux = 4
        mine = need_atm.shape[0]
        half = mine // PAIR
        owners = half * nsub
        entries = mine * nsub
        fields_a, acells = atm_state.shape
        fields_o, ocells = ocn_state.shape
        obl = ocells // blk
        owned = acells // blk
        cells = nb * blk
        dma = pltpu.SemaphoreType.DMA
        fluxes = pl.pallas_call(
            functools.partial(kernel, ntile, nsub, blk),
            out_shape=(
                pltpu.VMEM((nflux, acells), F32),
                pltpu.VMEM((nflux, ocells), F32),
            ),
            in_specs=[pl.BlockSpec(memory_space=pltpu.HBM)] * 10,
            out_specs=(pl.BlockSpec(memory_space=pltpu.VMEM),) * 2,
            scratch_shapes=[
                pltpu.VMEM((owned, fields_a, blk), BF16),
                pltpu.VMEM((nsub, obl, fields_o, blk), BF16),
                pltpu.SMEM((mine,), jnp.int32),
                pltpu.SMEM((nb,), jnp.int32),
                pltpu.SMEM((nb,), jnp.int32),
                pltpu.SMEM((1,), jnp.int32),
                pltpu.VMEM((1, cells), jnp.int32),
                pltpu.VMEM((1, cells), F32),
                pltpu.VMEM((nb, blk, blk), BF16),
                pltpu.VMEM((nb, blk, blk), BF16),
                pltpu.VMEM((half, owned, fields_a, blk), BF16),
                pltpu.VMEM((entries, fields_a, blk), BF16),
                pltpu.VMEM((half, 1, blk), jnp.int32),
                pltpu.VMEM((owners, 1, blk), jnp.int32),
                pltpu.VMEM((owners, PAIR, blk), F32),
                pltpu.VMEM((nsub, owners, PAIR, blk), F32),
                pltpu.VMEM((owners, PAIR * nflux, blk), F32),
                pltpu.VMEM((nsub, owners, PAIR * nflux, blk), F32),
                pltpu.VMEM((obl, ROWS, blk), F32),
                pltpu.VMEM((obl, ROWS, blk), F32),
                dma((8,)),
                dma((owned + obl,)),
                dma((half,)),
                dma((half,)),
                dma((half * nsub,)),
                dma((owners,)),
                dma(()),
                dma(()),
                dma(()),
                dma(()),
                dma((owners, nsub)),
                dma((nsub, owners)),
                dma((owners, nsub)),
                dma((nsub, owners)),
                dma(()),
                dma(()),
                dma(()),
            ],
            compiler_params=pltpu.CompilerParams(collective_id=0, has_side_effects=True),
        )(
            atm_state, ocn_state, need_atm, xb_need, xb_ocn, xb_count,
            sea_mask.reshape(1, cells), cell_area.reshape(1, cells), w_atm, w_ocn,
        )
        return pl.pallas_call(
            write_out,
            out_shape=tuple(jax.ShapeDtypeStruct(f.shape, F32) for f in fluxes),
            in_specs=[pl.BlockSpec(memory_space=pltpu.VMEM)] * 2,
            out_specs=(pl.BlockSpec(memory_space=pltpu.HBM),) * 2,
            scratch_shapes=[dma((2,))],
            compiler_params=pltpu.CompilerParams(vmem_limit_bytes=2**20),
        )(*fluxes)

    spread_all = P(("tile", "sub"))
    weights = P(("tile", "sub"), None, None)
    return jax.shard_map(
        per_device,
        mesh=mesh,
        in_specs=(
            P(None, ("member", "tile")),
            P(None, ("member", "tile", "sub")),
            spread_all, spread_all, spread_all, spread_all, spread_all, spread_all,
            weights, weights,
        ),
        out_specs=(P(None, ("member", "tile")), P(None, ("member", "tile", "sub"))),
        check_vma=False,
    )
```

```python
import functools

import jax
import jax.numpy as jnp
from jax import lax
from jax.experimental import pallas as pl
from jax.experimental.pallas import tpu as pltpu
from jax.sharding import PartitionSpec as P

MESH = pl.DeviceIdType.MESH
ROWS = 8
PAIR = 2
F32 = jnp.float32
BF16 = jnp.bfloat16
TRANSPOSED = (((1,), (1,)), ((), ()))


def split(value):
    high = value.astype(BF16)
    low = (value - high.astype(F32)).astype(BF16)
    return high, low


def kernel(
    ntile, nsub, blk,
    state_hbm, ocean_hbm, need_hbm, xbn_hbm, xbo_hbm, count_hbm, sea_hbm, area_hbm, wa_hbm, wo_hbm,
    atm_out, ocn_out,
    state, octab, need, xbn, xbo, count, sea, area, wa, wo,
    table, picked, rows_send, rows_recv, area_send, area_recv, sums_send, sums_recv, oc_send, oc_recv,
    load_sem, block_sem, push_ssem, push_rsem, row_ssem, row_rsem, oc_ssem, oc_rsem,
    pick_ssem, pick_rsem, area_ssem, area_rsem, sum_ssem, sum_rsem, ob_ssem, ob_rsem, keep_sem,
):
    me = lax.axis_index("tile")
    core = lax.axis_index("sub")
    other = 1 - core
    nb = wa.shape[0]
    mine = need.shape[0]
    half = mine // PAIR
    owners = half * nsub
    entries = mine * nsub
    owned = state.shape[0]
    obl = octab.shape[1]
    nflux = atm_out.shape[0]
    flux_lanes = owners * PAIR * nflux

    def offset(i):
        return ntile // 2 if i == owners - 1 else i - owners // 2 + 1

    def tile_at(delta):
        return lax.rem(me + delta + ntile, ntile)

    zero_i = [i for i in range(owners) if offset(i) == 0][0]

    local = [
        pltpu.make_async_copy(src, dst, load_sem.at[k])
        for k, (src, dst) in enumerate(
            [
                (need_hbm, need),
                (wo_hbm, wo),
                (wa_hbm, wa),
                (xbo_hbm, xbo),
                (xbn_hbm, xbn),
                (count_hbm, count),
                (sea_hbm, sea),
                (area_hbm, area),
            ]
        )
    ]
    blocks = [
        pltpu.make_async_copy(
            state_hbm.at[:, pl.ds(n * blk, blk)], state.at[n], block_sem.at[n]
        )
        for n in range(owned)
    ] + [
        pltpu.make_async_copy(
            ocean_hbm.at[:, pl.ds(n * blk, blk)], octab.at[core, n], block_sem.at[owned + n]
        )
        for n in range(obl)
    ]
    for copy in blocks + local:
        copy.start()

    barrier = pltpu.get_barrier_semaphore()
    for i in range(owners):
        for c in range(nsub):
            if i == zero_i:
                continue
            pl.semaphore_signal(
                barrier, inc=1, device_id={"tile": tile_at(offset(i)), "sub": c}, device_id_type=MESH
            )
    pl.semaphore_signal(barrier, inc=1, device_id={"tile": me, "sub": other}, device_id_type=MESH)

    local[0].wait()
    lane = lax.broadcasted_iota(jnp.int32, (1, blk), 1)
    odd = jnp.where(lane < flux_lanes, lax.rem(lane // nflux, PAIR), lax.rem(lane, PAIR))
    for k in range(half):
        first = lax.rem(need[PAIR * k], owned)
        second = lax.rem(need[PAIR * k + 1], owned)
        rows_send[k] = jnp.where(odd == 0, first, second)
    for copy in blocks:
        copy.wait()
    pl.semaphore_wait(barrier, owners * nsub - 1)

    def delta_of(k):
        i = core * half + k
        return jnp.where(i == owners - 1, ntile // 2, i - owners // 2 + 1)

    deltas = [delta_of(k) for k in range(half)]

    def push_of(k, delta):
        return pltpu.make_async_remote_copy(
            src_ref=state,
            dst_ref=table.at[k],
            send_sem=push_ssem.at[k],
            recv_sem=push_rsem.at[k],
            device_id={"tile": tile_at(-delta), "sub": core},
            device_id_type=MESH,
        )

    pushes = [push_of(k, deltas[k]) for k in range(half)]
    keep = pltpu.make_async_copy(state, table.at[zero_i % half], keep_sem)
    zero_core = zero_i // half
    far = [jnp.abs(tile_at(-delta) - me) for delta in deltas]
    for rank in range(half):
        pick = jnp.int32(0)
        for k in range(half):
            ahead = jnp.int32(0)
            for o in range(half):
                if o != k:
                    first = far[o] >= far[k] if o < k else far[o] > far[k]
                    ahead = ahead + jnp.where(first, 1, 0)
            pick = pick + jnp.where(ahead == rank, k, 0)
        push = push_of(pick, delta_of(pick))
        if rank == half - 1:
            @pl.when(core == zero_core)
            def _():
                keep.start()

            @pl.when(core != zero_core)
            def _(push=push):
                push.start()
        else:
            push.start()
    oc_copy = pltpu.make_async_remote_copy(
        src_ref=octab.at[core],
        dst_ref=octab.at[core],
        send_sem=oc_ssem,
        recv_sem=oc_rsem,
        device_id={"tile": me, "sub": other},
        device_id_type=MESH,
    )
    oc_copy.start()

    row_copies = []
    for k in range(half):
        slot = core * half + k
        for c in range(nsub):
            row_copies.append(
                pltpu.make_async_remote_copy(
                    src_ref=rows_send.at[k],
                    dst_ref=rows_recv.at[slot],
                    send_sem=row_ssem.at[k * nsub + c],
                    recv_sem=row_rsem.at[slot],
                    device_id={"tile": tile_at(deltas[k]), "sub": c},
                    device_id_type=MESH,
                )
            )
            copy = row_copies[-1]
            if k == zero_i % half:
                here = jnp.logical_and(core == zero_core, core == c)

                @pl.when(here)
                def _(k=k):
                    rows_recv[zero_i] = rows_send[k]

                @pl.when(jnp.logical_not(here))
                def _(copy=copy):
                    copy.start()
            else:
                copy.start()

    ones = jnp.ones((ROWS, blk), BF16)
    local[1].wait()
    local[3].wait()
    oc_copy.wait_recv()
    oxs = []
    for b in range(nb):
        m = xbo[b]
        cells = octab[lax.div(m, obl), lax.rem(m, obl)]
        w = wo[b]
        top = lax.dot_general(cells, w, TRANSPOSED, preferred_element_type=F32)
        den = lax.dot_general(ones, w, TRANSPOSED, preferred_element_type=F32)
        oxs.append(top / den[: top.shape[0]])
    ox = jnp.concatenate(oxs, axis=1)
    sst, uo, vo, oa = [ox[f : f + 1] for f in range(4)]
    albedo = 0.06 + 0.05 * (1.0 + jnp.tanh(0.5 * oa))
    local[2].wait()
    dens = jnp.concatenate(
        [lax.dot_general(ones, wa[b], TRANSPOSED, preferred_element_type=F32) for b in range(nb)],
        axis=1,
    )
    rden = 1.0 / dens
    for k in (4, 5, 6, 7):
        local[k].wait()
    cell = lax.broadcasted_iota(jnp.int32, (1, nb * blk), 1)
    weighted = jnp.where(cell < count[0] * blk, area[...], 0.0)
    wet = weighted * sea[...].astype(F32)

    def spread(both, w, index, number, step, shift):
        totals = [None] * number
        for b in range(nb):
            prod = jnp.dot(both[:, b * blk : (b + 1) * blk], w[b], preferred_element_type=F32)
            prod = prod[:ROWS] + prod[ROWS:]
            at = index[b] - shift
            for n in range(number):
                term = jnp.where(at == n * step, prod, 0.0)
                totals[n] = term if totals[n] is None else totals[n] + term
        return totals

    def send_owners(src, dst, ssem, rsem):
        copies = []
        for i in sorted(range(owners), key=lambda i: -abs(offset(i))):
            for c in range(nsub):
                if i == zero_i and c > 0:
                    continue
                copy = pltpu.make_async_remote_copy(
                    src_ref=src.at[i],
                    dst_ref=dst.at[core, i],
                    send_sem=ssem.at[i, c],
                    recv_sem=rsem.at[core, i],
                    device_id={"tile": tile_at(offset(i)), "sub": other if i == zero_i else c},
                    device_id_type=MESH,
                )
                copy.start()
                copies.append(copy)
        return copies

    row_id = lax.broadcasted_iota(jnp.int32, (ROWS, blk), 0)
    areas = jnp.concatenate(split(jnp.broadcast_to(weighted, (ROWS, nb * blk))), axis=0)
    totals = spread(areas, wa, xbn, owners, PAIR, lax.rem(row_id, PAIR))
    for i in range(owners):
        area_send[i] = totals[i][:PAIR]
    area_recv[core, zero_i] = totals[zero_i][:PAIR]

    for k in range(half):
        if k == zero_i % half:
            @pl.when(core == zero_core)
            def _():
                keep.wait()

            @pl.when(core != zero_core)
            def _(k=k):
                pushes[k].wait_recv()
        else:
            pushes[k].wait_recv()
    for e in range(mine):
        picked[core * mine + e] = table[e // PAIR, lax.rem(need[e], owned)]
    part = picked.at[pl.ds(core * mine, mine)]
    pick_copy = pltpu.make_async_remote_copy(
        src_ref=part,
        dst_ref=part,
        send_sem=pick_ssem,
        recv_sem=pick_rsem,
        device_id={"tile": me, "sub": other},
        device_id_type=MESH,
    )
    pick_copy.start()
    area_copies = send_owners(area_send, area_recv, area_ssem, area_rsem)
    pick_copy.wait_recv()
    ax = jnp.concatenate(
        [
            lax.dot_general(picked[xbn[b]], wa[b], TRANSPOSED, preferred_element_type=F32)
            for b in range(nb)
        ],
        axis=1,
    )
    ax = ax * rden
    ta, qa, ua, va, ps, sw, lw, pr = [ax[f : f + 1] for f in range(8)]

    du = ua - uo
    dv = va - vo
    speed = jnp.sqrt(du * du + dv * dv + 1.0)
    cd = (0.3 + 0.1 * jnp.tanh(ps)) * speed
    sens = cd * (sst - ta)
    lat = cd * (0.5 * sst - qa)
    taux = cd * du
    tauy = cd * dv
    pad = jnp.zeros((ROWS - 5, nb * blk), F32)
    fluxes = [sens * wet, lat * wet, taux * wet, tauy * wet]
    both = jnp.concatenate(split(jnp.concatenate(fluxes * PAIR, axis=0)), axis=0)
    totals = spread(both, wa, xbn, owners, PAIR, row_id // nflux)
    for i in range(owners):
        sums_send[i] = totals[i]
    sum_copies = send_owners(sums_send, sums_recv, sum_ssem, sum_rsem)
    sums_recv[core, zero_i] = totals[zero_i]

    heat = (1.0 - albedo) * sw + lw - 0.2 * sst - sens - lat
    fresh = pr - 0.5 * lat
    pad = jnp.zeros((ROWS - nflux - 1, nb * blk), F32)
    ocn_terms = jnp.concatenate([heat * wet, taux * wet, tauy * wet, fresh * wet, wet, pad], 0)
    ototals = spread(jnp.concatenate(split(ocn_terms), axis=0), wo, xbo, obl * nsub, 1, 0)
    own = []
    for m in range(obl):
        low, high = ototals[m], ototals[obl + m]
        oc_send[m] = jnp.where(core == 0, high, low)
        own.append(jnp.where(core == 0, low, high))
    ob_copy = pltpu.make_async_remote_copy(
        src_ref=oc_send,
        dst_ref=oc_recv,
        send_sem=ob_ssem,
        recv_sem=ob_rsem,
        device_id={"tile": me, "sub": other},
        device_id_type=MESH,
    )
    ob_copy.start()

    def recv_desc(src, dst, ssem, rsem):
        return pltpu.make_async_remote_copy(
            src_ref=src, dst_ref=dst, send_sem=ssem, recv_sem=rsem,
            device_id={"tile": me, "sub": other}, device_id_type=MESH,
        )

    for i in range(owners):
        desc = recv_desc(rows_send.at[0], rows_recv.at[i], row_ssem.at[0], row_rsem.at[i])
        if i == zero_i:
            @pl.when(core != zero_core)
            def _(desc=desc):
                desc.wait_recv()
        else:
            desc.wait_recv()
    places = jnp.concatenate([rows_recv[i] for i in range(owners)], axis=0)
    lanes = lax.broadcasted_iota(jnp.int32, (owners, blk), 1)
    slot_of = jnp.where(
        lanes < flux_lanes, lanes // (PAIR * nflux), (lanes - flux_lanes) // PAIR
    )
    mask = slot_of == lax.broadcasted_iota(jnp.int32, (owners, blk), 0)
    place = jnp.sum(jnp.where(mask, places, 0), axis=0, keepdims=True)
    down = lax.broadcasted_iota(jnp.int32, (owned * nflux, blk), 0)
    across = lax.broadcasted_iota(jnp.int32, (owned * nflux, blk), 1)
    hit = jnp.logical_and(
        down // nflux == place,
        jnp.logical_or(across >= flux_lanes, lax.rem(down, nflux) == lax.rem(across, nflux)),
    )
    landing = jnp.where(hit, 1.0, 0.0)
    landing_flux = landing[:, :flux_lanes].astype(BF16)
    landing_area = landing[:, flux_lanes : flux_lanes + owners * PAIR].astype(BF16)

    def land(landing, value):
        high, low = split(value)
        return jnp.dot(landing, high, preferred_element_type=F32) + jnp.dot(
            landing, low, preferred_element_type=F32
        )

    def wait_owners(src, dst, ssem, rsem):
        for c in range(nsub):
            for i in range(owners):
                desc = recv_desc(src.at[i], dst.at[c, i], ssem.at[i, 0], rsem.at[c, i])
                if i == zero_i:
                    @pl.when(core != c)
                    def _(desc=desc):
                        desc.wait_recv()
                else:
                    desc.wait_recv()

    ob_copy.wait_recv()
    for m in range(obl):
        tot = own[m] + oc_recv[m]
        ocn_out[:, m * blk : (m + 1) * blk] = tot[:nflux] / jnp.maximum(tot[nflux : nflux + 1], 1.0)

    wait_owners(area_send, area_recv, area_ssem, area_rsem)
    arrived = jnp.concatenate([area_recv[0, i] + area_recv[1, i] for i in range(owners)], axis=0)
    scale = 1.0 / jnp.maximum(land(landing_area, arrived), 1.0)

    wait_owners(sums_send, sums_recv, sum_ssem, sum_rsem)
    arrived = (sums_recv[0] + sums_recv[1]).reshape(flux_lanes, blk)
    final = land(landing_flux, arrived) * scale
    for a in range(owned):
        atm_out[:, a * blk : (a + 1) * blk] = final[a * nflux : (a + 1) * nflux]

    for k in range(half):
        if k == zero_i % half:
            @pl.when(core != zero_core)
            def _(k=k):
                pushes[k].wait_send()
        else:
            pushes[k].wait_send()
    for k in range(half):
        for c in range(nsub):
            copy = row_copies[k * nsub + c]
            if k == zero_i % half:
                @pl.when(jnp.logical_not(jnp.logical_and(core == zero_core, core == c)))
                def _(copy=copy):
                    copy.wait_send()
            else:
                copy.wait_send()
    oc_copy.wait_send()
    pick_copy.wait_send()
    for copy in area_copies + sum_copies:
        copy.wait_send()
    ob_copy.wait_send()


def write_out(atm, ocn, atm_hbm, ocn_hbm, sem):
    copies = [
        pltpu.make_async_copy(src, dst, sem.at[k])
        for k, (src, dst) in enumerate([(atm, atm_hbm), (ocn, ocn_hbm)])
    ]
    for copy in copies:
        copy.start()
    for copy in copies:
        copy.wait()


def solution(mesh):
    ntile, nsub = mesh.shape["tile"], mesh.shape["sub"]

    def per_device(
        atm_state, ocn_state, need_atm, xb_need, xb_ocn, xb_count, sea_mask, cell_area, w_atm, w_ocn
    ):
        nb, blk, _ = w_atm.shape
        nflux = 4
        mine = need_atm.shape[0]
        half = mine // PAIR
        owners = half * nsub
        entries = mine * nsub
        fields_a, acells = atm_state.shape
        fields_o, ocells = ocn_state.shape
        obl = ocells // blk
        owned = acells // blk
        cells = nb * blk
        dma = pltpu.SemaphoreType.DMA
        fluxes = pl.pallas_call(
            functools.partial(kernel, ntile, nsub, blk),
            out_shape=(
                pltpu.VMEM((nflux, acells), F32),
                pltpu.VMEM((nflux, ocells), F32),
            ),
            in_specs=[pl.BlockSpec(memory_space=pltpu.HBM)] * 10,
            out_specs=(pl.BlockSpec(memory_space=pltpu.VMEM),) * 2,
            scratch_shapes=[
                pltpu.VMEM((owned, fields_a, blk), BF16),
                pltpu.VMEM((nsub, obl, fields_o, blk), BF16),
                pltpu.SMEM((mine,), jnp.int32),
                pltpu.SMEM((nb,), jnp.int32),
                pltpu.SMEM((nb,), jnp.int32),
                pltpu.SMEM((1,), jnp.int32),
                pltpu.VMEM((1, cells), jnp.int32),
                pltpu.VMEM((1, cells), F32),
                pltpu.VMEM((nb, blk, blk), BF16),
                pltpu.VMEM((nb, blk, blk), BF16),
                pltpu.VMEM((half, owned, fields_a, blk), BF16),
                pltpu.VMEM((entries, fields_a, blk), BF16),
                pltpu.VMEM((half, 1, blk), jnp.int32),
                pltpu.VMEM((owners, 1, blk), jnp.int32),
                pltpu.VMEM((owners, PAIR, blk), F32),
                pltpu.VMEM((nsub, owners, PAIR, blk), F32),
                pltpu.VMEM((owners, PAIR * nflux, blk), F32),
                pltpu.VMEM((nsub, owners, PAIR * nflux, blk), F32),
                pltpu.VMEM((obl, ROWS, blk), F32),
                pltpu.VMEM((obl, ROWS, blk), F32),
                dma((8,)),
                dma((owned + obl,)),
                dma((half,)),
                dma((half,)),
                dma((half * nsub,)),
                dma((owners,)),
                dma(()),
                dma(()),
                dma(()),
                dma(()),
                dma((owners, nsub)),
                dma((nsub, owners)),
                dma((owners, nsub)),
                dma((nsub, owners)),
                dma(()),
                dma(()),
                dma(()),
            ],
            compiler_params=pltpu.CompilerParams(collective_id=0, has_side_effects=True),
        )(
            atm_state, ocn_state, need_atm, xb_need, xb_ocn, xb_count,
            sea_mask.reshape(1, cells), cell_area.reshape(1, cells), w_atm, w_ocn,
        )
        return pl.pallas_call(
            write_out,
            out_shape=tuple(jax.ShapeDtypeStruct(f.shape, F32) for f in fluxes),
            in_specs=[pl.BlockSpec(memory_space=pltpu.VMEM)] * 2,
            out_specs=(pl.BlockSpec(memory_space=pltpu.HBM),) * 2,
            scratch_shapes=[dma((2,))],
            compiler_params=pltpu.CompilerParams(vmem_limit_bytes=2**20),
        )(*fluxes)

    spread_all = P(("tile", "sub"))
    weights = P(("tile", "sub"), None, None)
    return jax.shard_map(
        per_device,
        mesh=mesh,
        in_specs=(
            P(None, ("member", "tile")),
            P(None, ("member", "tile", "sub")),
            spread_all, spread_all, spread_all, spread_all, spread_all, spread_all,
            weights, weights,
        ),
        out_specs=(P(None, ("member", "tile")), P(None, ("member", "tile", "sub"))),
        check_vma=False,
    )
```

```python
import functools

import jax
import jax.numpy as jnp
from jax import lax
from jax.experimental import pallas as pl
from jax.experimental.pallas import tpu as pltpu
from jax.sharding import PartitionSpec as P

MESH = pl.DeviceIdType.MESH
ROWS = 8
PAIR = 2
F32 = jnp.float32
BF16 = jnp.bfloat16
TRANSPOSED = (((1,), (1,)), ((), ()))


def split(value):
    high = value.astype(BF16)
    low = (value - high.astype(F32)).astype(BF16)
    return high, low


def kernel(
    ntile, nsub, blk,
    state_hbm, ocean_hbm, need_hbm, xbn_hbm, xbo_hbm, count_hbm, sea_hbm, area_hbm, wa_hbm, wo_hbm,
    atm_out, ocn_out,
    state, octab, need, xbn, xbo, count, sea, area, wa, wo,
    table, picked, rows_send, rows_recv, area_send, area_recv, sums_send, sums_recv, oc_send, oc_recv,
    load_sem, block_sem, push_ssem, push_rsem, row_ssem, row_rsem, oc_ssem, oc_rsem,
    pick_ssem, pick_rsem, area_ssem, area_rsem, sum_ssem, sum_rsem, ob_ssem, ob_rsem, keep_sem,
):
    me = lax.axis_index("tile")
    core = lax.axis_index("sub")
    other = 1 - core
    nb = wa.shape[0]
    mine = need.shape[0]
    half = mine // PAIR
    owners = half * nsub
    entries = mine * nsub
    owned = state.shape[0]
    obl = octab.shape[1]
    nflux = atm_out.shape[0]
    flux_lanes = owners * PAIR * nflux

    def offset(i):
        return ntile // 2 if i == owners - 1 else i - owners // 2 + 1

    def tile_at(delta):
        return lax.rem(me + delta + ntile, ntile)

    zero_i = [i for i in range(owners) if offset(i) == 0][0]

    barrier = pltpu.get_barrier_semaphore()
    for i in sorted(range(owners), key=lambda i: -abs(offset(i))):
        for c in range(nsub):
            if i == zero_i:
                continue
            pl.semaphore_signal(
                barrier, inc=1, device_id={"tile": tile_at(offset(i)), "sub": c}, device_id_type=MESH
            )
    pl.semaphore_signal(barrier, inc=1, device_id={"tile": me, "sub": other}, device_id_type=MESH)

    local = [
        pltpu.make_async_copy(src, dst, load_sem.at[k])
        for k, (src, dst) in enumerate(
            [
                (need_hbm, need),
                (wo_hbm, wo),
                (wa_hbm, wa),
                (xbo_hbm, xbo),
                (xbn_hbm, xbn),
                (count_hbm, count),
                (sea_hbm, sea),
                (area_hbm, area),
            ]
        )
    ]
    blocks = [
        pltpu.make_async_copy(
            state_hbm.at[:, pl.ds(n * blk, blk)], state.at[n], block_sem.at[n]
        )
        for n in range(owned)
    ] + [
        pltpu.make_async_copy(
            ocean_hbm.at[:, pl.ds(n * blk, blk)], octab.at[core, n], block_sem.at[owned + n]
        )
        for n in range(obl)
    ]
    for copy in blocks + local:
        copy.start()

    local[0].wait()
    lane = lax.broadcasted_iota(jnp.int32, (1, blk), 1)
    odd = jnp.where(lane < flux_lanes, lax.rem(lane // nflux, PAIR), lax.rem(lane, PAIR))
    for k in range(half):
        first = lax.rem(need[PAIR * k], owned)
        second = lax.rem(need[PAIR * k + 1], owned)
        rows_send[k] = jnp.where(odd == 0, first, second)
    for copy in blocks:
        copy.wait()
    pl.semaphore_wait(barrier, owners * nsub - 1)

    def delta_of(k):
        i = core * half + k
        return jnp.where(i == owners - 1, ntile // 2, i - owners // 2 + 1)

    deltas = [delta_of(k) for k in range(half)]

    def push_of(k, delta):
        return pltpu.make_async_remote_copy(
            src_ref=state,
            dst_ref=table.at[k],
            send_sem=push_ssem.at[k],
            recv_sem=push_rsem.at[k],
            device_id={"tile": tile_at(-delta), "sub": core},
            device_id_type=MESH,
        )

    pushes = [push_of(k, deltas[k]) for k in range(half)]
    keep = pltpu.make_async_copy(state, table.at[zero_i % half], keep_sem)
    zero_core = zero_i // half
    far = [jnp.abs(tile_at(-delta) - me) for delta in deltas]
    for rank in range(half):
        pick = jnp.int32(0)
        for k in range(half):
            ahead = jnp.int32(0)
            for o in range(half):
                if o != k:
                    first = far[o] >= far[k] if o < k else far[o] > far[k]
                    ahead = ahead + jnp.where(first, 1, 0)
            pick = pick + jnp.where(ahead == rank, k, 0)
        push = push_of(pick, delta_of(pick))
        if rank == half - 1:
            @pl.when(core == zero_core)
            def _():
                keep.start()

            @pl.when(core != zero_core)
            def _(push=push):
                push.start()
        else:
            push.start()
    oc_copy = pltpu.make_async_remote_copy(
        src_ref=octab.at[core],
        dst_ref=octab.at[core],
        send_sem=oc_ssem,
        recv_sem=oc_rsem,
        device_id={"tile": me, "sub": other},
        device_id_type=MESH,
    )
    oc_copy.start()

    row_copies = []
    for k in range(half):
        slot = core * half + k
        for c in range(nsub):
            row_copies.append(
                pltpu.make_async_remote_copy(
                    src_ref=rows_send.at[k],
                    dst_ref=rows_recv.at[slot],
                    send_sem=row_ssem.at[k * nsub + c],
                    recv_sem=row_rsem.at[slot],
                    device_id={"tile": tile_at(deltas[k]), "sub": c},
                    device_id_type=MESH,
                )
            )
            copy = row_copies[-1]
            if k == zero_i % half:
                here = jnp.logical_and(core == zero_core, core == c)

                @pl.when(here)
                def _(k=k):
                    rows_recv[zero_i] = rows_send[k]

                @pl.when(jnp.logical_not(here))
                def _(copy=copy):
                    copy.start()
            else:
                copy.start()

    ones = jnp.ones((ROWS, blk), BF16)
    local[1].wait()
    local[3].wait()
    oc_copy.wait_recv()
    oxs = []
    for b in range(nb):
        m = xbo[b]
        cells = octab[lax.div(m, obl), lax.rem(m, obl)]
        w = wo[b]
        top = lax.dot_general(cells, w, TRANSPOSED, preferred_element_type=F32)
        den = lax.dot_general(ones, w, TRANSPOSED, preferred_element_type=F32)
        oxs.append(top / den[: top.shape[0]])
    ox = jnp.concatenate(oxs, axis=1)
    sst, uo, vo, oa = [ox[f : f + 1] for f in range(4)]
    albedo = 0.06 + 0.05 * (1.0 + jnp.tanh(0.5 * oa))
    local[2].wait()
    dens = jnp.concatenate(
        [lax.dot_general(ones, wa[b], TRANSPOSED, preferred_element_type=F32) for b in range(nb)],
        axis=1,
    )
    rden = 1.0 / dens
    for k in (4, 5, 6, 7):
        local[k].wait()
    cell = lax.broadcasted_iota(jnp.int32, (1, nb * blk), 1)
    weighted = jnp.where(cell < count[0] * blk, area[...], 0.0)
    wet = weighted * sea[...].astype(F32)

    def spread(both, w, index, number, step, shift):
        totals = [None] * number
        for b in range(nb):
            prod = jnp.dot(both[:, b * blk : (b + 1) * blk], w[b], preferred_element_type=F32)
            prod = prod[:ROWS] + prod[ROWS:]
            at = index[b] - shift
            for n in range(number):
                term = jnp.where(at == n * step, prod, 0.0)
                totals[n] = term if totals[n] is None else totals[n] + term
        return totals

    def send_owners(src, dst, ssem, rsem):
        copies = []
        for i in sorted(range(owners), key=lambda i: -abs(offset(i))):
            for c in range(nsub):
                if i == zero_i and c > 0:
                    continue
                copy = pltpu.make_async_remote_copy(
                    src_ref=src.at[i],
                    dst_ref=dst.at[core, i],
                    send_sem=ssem.at[i, c],
                    recv_sem=rsem.at[core, i],
                    device_id={"tile": tile_at(offset(i)), "sub": other if i == zero_i else c},
                    device_id_type=MESH,
                )
                copy.start()
                copies.append(copy)
        return copies

    row_id = lax.broadcasted_iota(jnp.int32, (ROWS, blk), 0)
    areas = jnp.concatenate(split(jnp.broadcast_to(weighted, (ROWS, nb * blk))), axis=0)
    totals = spread(areas, wa, xbn, owners, PAIR, lax.rem(row_id, PAIR))
    for i in range(owners):
        area_send[i] = totals[i][:PAIR]
    area_recv[core, zero_i] = totals[zero_i][:PAIR]

    for k in range(half):
        if k == zero_i % half:
            @pl.when(core == zero_core)
            def _():
                keep.wait()

            @pl.when(core != zero_core)
            def _(k=k):
                pushes[k].wait_recv()
        else:
            pushes[k].wait_recv()
    for e in range(mine):
        picked[core * mine + e] = table[e // PAIR, lax.rem(need[e], owned)]
    part = picked.at[pl.ds(core * mine, mine)]
    pick_copy = pltpu.make_async_remote_copy(
        src_ref=part,
        dst_ref=part,
        send_sem=pick_ssem,
        recv_sem=pick_rsem,
        device_id={"tile": me, "sub": other},
        device_id_type=MESH,
    )
    pick_copy.start()
    area_copies = send_owners(area_send, area_recv, area_ssem, area_rsem)
    pick_copy.wait_recv()
    ax = jnp.concatenate(
        [
            lax.dot_general(picked[xbn[b]], wa[b], TRANSPOSED, preferred_element_type=F32)
            for b in range(nb)
        ],
        axis=1,
    )
    ax = ax * rden
    ta, qa, ua, va, ps, sw, lw, pr = [ax[f : f + 1] for f in range(8)]

    du = ua - uo
    dv = va - vo
    speed = jnp.sqrt(du * du + dv * dv + 1.0)
    cd = (0.3 + 0.1 * jnp.tanh(ps)) * speed
    sens = cd * (sst - ta)
    lat = cd * (0.5 * sst - qa)
    taux = cd * du
    tauy = cd * dv
    pad = jnp.zeros((ROWS - 5, nb * blk), F32)
    fluxes = [sens * wet, lat * wet, taux * wet, tauy * wet]
    both = jnp.concatenate(split(jnp.concatenate(fluxes * PAIR, axis=0)), axis=0)
    totals = spread(both, wa, xbn, owners, PAIR, row_id // nflux)
    for i in range(owners):
        sums_send[i] = totals[i]
    sum_copies = send_owners(sums_send, sums_recv, sum_ssem, sum_rsem)
    sums_recv[core, zero_i] = totals[zero_i]

    heat = (1.0 - albedo) * sw + lw - 0.2 * sst - sens - lat
    fresh = pr - 0.5 * lat
    pad = jnp.zeros((ROWS - nflux - 1, nb * blk), F32)
    ocn_terms = jnp.concatenate([heat * wet, taux * wet, tauy * wet, fresh * wet, wet, pad], 0)
    ototals = spread(jnp.concatenate(split(ocn_terms), axis=0), wo, xbo, obl * nsub, 1, 0)
    own = []
    for m in range(obl):
        low, high = ototals[m], ototals[obl + m]
        oc_send[m] = jnp.where(core == 0, high, low)
        own.append(jnp.where(core == 0, low, high))
    ob_copy = pltpu.make_async_remote_copy(
        src_ref=oc_send,
        dst_ref=oc_recv,
        send_sem=ob_ssem,
        recv_sem=ob_rsem,
        device_id={"tile": me, "sub": other},
        device_id_type=MESH,
    )
    ob_copy.start()

    def recv_desc(src, dst, ssem, rsem):
        return pltpu.make_async_remote_copy(
            src_ref=src, dst_ref=dst, send_sem=ssem, recv_sem=rsem,
            device_id={"tile": me, "sub": other}, device_id_type=MESH,
        )

    for i in range(owners):
        desc = recv_desc(rows_send.at[0], rows_recv.at[i], row_ssem.at[0], row_rsem.at[i])
        if i == zero_i:
            @pl.when(core != zero_core)
            def _(desc=desc):
                desc.wait_recv()
        else:
            desc.wait_recv()
    places = jnp.concatenate([rows_recv[i] for i in range(owners)], axis=0)
    lanes = lax.broadcasted_iota(jnp.int32, (owners, blk), 1)
    slot_of = jnp.where(
        lanes < flux_lanes, lanes // (PAIR * nflux), (lanes - flux_lanes) // PAIR
    )
    mask = slot_of == lax.broadcasted_iota(jnp.int32, (owners, blk), 0)
    place = jnp.sum(jnp.where(mask, places, 0), axis=0, keepdims=True)
    down = lax.broadcasted_iota(jnp.int32, (owned * nflux, blk), 0)
    across = lax.broadcasted_iota(jnp.int32, (owned * nflux, blk), 1)
    hit = jnp.logical_and(
        down // nflux == place,
        jnp.logical_or(across >= flux_lanes, lax.rem(down, nflux) == lax.rem(across, nflux)),
    )
    landing = jnp.where(hit, 1.0, 0.0)
    landing_flux = landing[:, :flux_lanes].astype(BF16)
    landing_area = landing[:, flux_lanes : flux_lanes + owners * PAIR].astype(BF16)

    def land(landing, value):
        high, low = split(value)
        return jnp.dot(landing, high, preferred_element_type=F32) + jnp.dot(
            landing, low, preferred_element_type=F32
        )

    def wait_owners(src, dst, ssem, rsem):
        for c in range(nsub):
            for i in range(owners):
                desc = recv_desc(src.at[i], dst.at[c, i], ssem.at[i, 0], rsem.at[c, i])
                if i == zero_i:
                    @pl.when(core != c)
                    def _(desc=desc):
                        desc.wait_recv()
                else:
                    desc.wait_recv()

    ob_copy.wait_recv()
    for m in range(obl):
        tot = own[m] + oc_recv[m]
        ocn_out[:, m * blk : (m + 1) * blk] = tot[:nflux] / jnp.maximum(tot[nflux : nflux + 1], 1.0)

    wait_owners(area_send, area_recv, area_ssem, area_rsem)
    arrived = jnp.concatenate([area_recv[0, i] + area_recv[1, i] for i in range(owners)], axis=0)
    scale = 1.0 / jnp.maximum(land(landing_area, arrived), 1.0)

    wait_owners(sums_send, sums_recv, sum_ssem, sum_rsem)
    arrived = (sums_recv[0] + sums_recv[1]).reshape(flux_lanes, blk)
    final = land(landing_flux, arrived) * scale
    for a in range(owned):
        atm_out[:, a * blk : (a + 1) * blk] = final[a * nflux : (a + 1) * nflux]

    for k in range(half):
        if k == zero_i % half:
            @pl.when(core != zero_core)
            def _(k=k):
                pushes[k].wait_send()
        else:
            pushes[k].wait_send()
    for k in range(half):
        for c in range(nsub):
            copy = row_copies[k * nsub + c]
            if k == zero_i % half:
                @pl.when(jnp.logical_not(jnp.logical_and(core == zero_core, core == c)))
                def _(copy=copy):
                    copy.wait_send()
            else:
                copy.wait_send()
    oc_copy.wait_send()
    pick_copy.wait_send()
    for copy in area_copies + sum_copies:
        copy.wait_send()
    ob_copy.wait_send()


def write_out(atm, ocn, atm_hbm, ocn_hbm, sem):
    copies = [
        pltpu.make_async_copy(src, dst, sem.at[k])
        for k, (src, dst) in enumerate([(atm, atm_hbm), (ocn, ocn_hbm)])
    ]
    for copy in copies:
        copy.start()
    for copy in copies:
        copy.wait()


def solution(mesh):
    ntile, nsub = mesh.shape["tile"], mesh.shape["sub"]

    def per_device(
        atm_state, ocn_state, need_atm, xb_need, xb_ocn, xb_count, sea_mask, cell_area, w_atm, w_ocn
    ):
        nb, blk, _ = w_atm.shape
        nflux = 4
        mine = need_atm.shape[0]
        half = mine // PAIR
        owners = half * nsub
        entries = mine * nsub
        fields_a, acells = atm_state.shape
        fields_o, ocells = ocn_state.shape
        obl = ocells // blk
        owned = acells // blk
        cells = nb * blk
        dma = pltpu.SemaphoreType.DMA
        fluxes = pl.pallas_call(
            functools.partial(kernel, ntile, nsub, blk),
            out_shape=(
                pltpu.VMEM((nflux, acells), F32),
                pltpu.VMEM((nflux, ocells), F32),
            ),
            in_specs=[pl.BlockSpec(memory_space=pltpu.HBM)] * 10,
            out_specs=(pl.BlockSpec(memory_space=pltpu.VMEM),) * 2,
            scratch_shapes=[
                pltpu.VMEM((owned, fields_a, blk), BF16),
                pltpu.VMEM((nsub, obl, fields_o, blk), BF16),
                pltpu.SMEM((mine,), jnp.int32),
                pltpu.SMEM((nb,), jnp.int32),
                pltpu.SMEM((nb,), jnp.int32),
                pltpu.SMEM((1,), jnp.int32),
                pltpu.VMEM((1, cells), jnp.int32),
                pltpu.VMEM((1, cells), F32),
                pltpu.VMEM((nb, blk, blk), BF16),
                pltpu.VMEM((nb, blk, blk), BF16),
                pltpu.VMEM((half, owned, fields_a, blk), BF16),
                pltpu.VMEM((entries, fields_a, blk), BF16),
                pltpu.VMEM((half, 1, blk), jnp.int32),
                pltpu.VMEM((owners, 1, blk), jnp.int32),
                pltpu.VMEM((owners, PAIR, blk), F32),
                pltpu.VMEM((nsub, owners, PAIR, blk), F32),
                pltpu.VMEM((owners, PAIR * nflux, blk), F32),
                pltpu.VMEM((nsub, owners, PAIR * nflux, blk), F32),
                pltpu.VMEM((obl, ROWS, blk), F32),
                pltpu.VMEM((obl, ROWS, blk), F32),
                dma((8,)),
                dma((owned + obl,)),
                dma((half,)),
                dma((half,)),
                dma((half * nsub,)),
                dma((owners,)),
                dma(()),
                dma(()),
                dma(()),
                dma(()),
                dma((owners, nsub)),
                dma((nsub, owners)),
                dma((owners, nsub)),
                dma((nsub, owners)),
                dma(()),
                dma(()),
                dma(()),
            ],
            compiler_params=pltpu.CompilerParams(collective_id=0, has_side_effects=True),
        )(
            atm_state, ocn_state, need_atm, xb_need, xb_ocn, xb_count,
            sea_mask.reshape(1, cells), cell_area.reshape(1, cells), w_atm, w_ocn,
        )
        return pl.pallas_call(
            write_out,
            out_shape=tuple(jax.ShapeDtypeStruct(f.shape, F32) for f in fluxes),
            in_specs=[pl.BlockSpec(memory_space=pltpu.VMEM)] * 2,
            out_specs=(pl.BlockSpec(memory_space=pltpu.HBM),) * 2,
            scratch_shapes=[dma((2,))],
            compiler_params=pltpu.CompilerParams(vmem_limit_bytes=2**20),
        )(*fluxes)

    spread_all = P(("tile", "sub"))
    weights = P(("tile", "sub"), None, None)
    return jax.shard_map(
        per_device,
        mesh=mesh,
        in_specs=(
            P(None, ("member", "tile")),
            P(None, ("member", "tile", "sub")),
            spread_all, spread_all, spread_all, spread_all, spread_all, spread_all,
            weights, weights,
        ),
        out_specs=(P(None, ("member", "tile")), P(None, ("member", "tile", "sub"))),
        check_vma=False,
    )
```
